512 devices in a mesh: hx: 4 (over y_hi), hy: 4 (over x), tok: 32 (over y_lo, z, core).
Axes of the slice: x: 4, y: 8 (y_hi: 4, y_lo: 2; y = y_hi * 2 + y_lo), z: 8, core: 2. Of those that a mesh axis runs over, the one named last changes fastest.
Arguments:
- stream_in: bfloat16 [8192, 4608], P('tok', ('hx', 'hy')), may hold values from -6 to 6
- before_gain: bfloat16 [4608], P(('hx', 'hy')), may hold values from 0.25 to 1.75
- after_gain: bfloat16 [4608], P(('hx', 'hy')), may hold values from 0.25 to 1.75
- feed_gain: bfloat16 [4608], P(('hx', 'hy')), may hold values from 0.25 to 1.75
- query_weight: bfloat16 [4608, 4096], P('tok', ('hx', 'hy')), may hold values from -1 to 1
- key_weight: bfloat16 [4608, 2048], P('tok', ('hx', 'hy')), may hold values from -64 to 64
- value_weight: bfloat16 [4608, 2048], P('tok', ('hx', 'hy')), may hold values from -0.09375 to 0.09375
- output_weight: bfloat16 [4096, 4608], P(('hx', 'hy'), 'tok'), may hold values from -0.09375 to 0.09375
- documents: int32 [8192], P('tok'), may hold values from 0 to 127, never falling along the last dimension, each value on 1 to 128 neighbouring positions
Outputs:
- residual: bfloat16 [8192, 4608], P('tok', ('hx', 'hy'))
- feed_input: bfloat16 [8192, 4608], P('tok', ('hx', 'hy'))
The draws below stay inside these ranges and needn't reach their ends.
Inputs may be any that keep to these rules, and one draw needn't show every extreme that they name: `documents`: ids never fall along the tokens; a document holds at most 128 tokens and may run across a sequence's end.
All inputs are finite; a program needn't handle non-finite values.
Results may differ from the reference program's by a relative error of at most 0.014.
The reference program's roundings to bfloat16 on the way count: a program that leaves them out, or rounds other values in their place, can miss the bound.
Values may be sent and summed in bfloat16 or wider, within the bound.
No kernel may reach another device: no remote copies, remote signals or barrier semaphores. Data moves between devices by JAX's collectives and lax.ppermute only.
A program may use at most 64 MiB of HBM per device.

```python
import math
import jax
import jax.numpy as jnp
import numpy as np
from jax import lax

D = 4608
QH = 32
KVH = 16
HEAD = 128
LENGTH = 256
TOKENS = 8192
DOCS = 128
N_HX = 4
N_HY = 4


def query_base(key):
    return jax.random.truncated_normal(jax.random.fold_in(key, 11), -6.0, 6.0, (D, QH * HEAD), jnp.float32) * D ** (-0.5)


def draw_query_weight(key, part):
    return query_base(key).astype(jnp.bfloat16)


def draw_key_weight(key, part):
    independent = jax.random.truncated_normal(jax.random.fold_in(key, 23), -6.0, 6.0, (D, KVH * HEAD), jnp.float32) * D ** (-0.5)
    return independent.astype(jnp.bfloat16)


def steps_of(stream_key, shape, split, smallest, high):
    def one(position, shards_of):
        heights = jax.random.uniform(jax.random.fold_in(jax.random.fold_in(stream_key, 6), position), (shards_of,), jnp.float32, smallest / len(split), high / len(split))
        return jnp.repeat(jnp.exp(heights), shape[position] // shards_of).reshape((-1,) + (1,) * (len(shape) - position - 1))

    level = one(*split[0])
    for cut in split[1:]:
        level = level * one(*cut)
    return level


def split_up(amount, total, bound, lean):
    weights = [(1 << 20) // math.isqrt(standing ** lean) + 1 for standing in range(2, amount + 1)]
    surplus, counts = total - bound - (amount - 1), [1] * (amount - 1)
    while surplus > 0:
        candidates = [i for i in range(amount - 1) if counts[i] < bound]
        whole, left = sum([weights[i] for i in candidates]), surplus
        for i in candidates:
            more = min(bound - counts[i], max(1, left * weights[i] // whole), surplus)
            counts[i] = counts[i] + more
            surplus = surplus - more
    return np.array([bound] + counts)


def uneven_parts(rng, amount, total, limit, skew):
    if amount == 2:
        one = jax.random.randint(rng, (), max(1, total - limit), min(limit, total - 1) + 1)
        return jnp.stack([one, total - one])
    lengths = jnp.asarray(split_up(amount, total, limit, skew), jnp.int32)
    pairs = (amount - 1) // 2
    donor, receiver = lengths[1:1 + 2 * pairs:2], lengths[2:2 + 2 * pairs:2]
    margin = jnp.minimum(donor - 1, limit - receiver)
    passed = jax.random.randint(jax.random.fold_in(rng, 1), (pairs,), 0, 1 << 20) % (margin + 1)
    lengths = lengths.at[1:1 + 2 * pairs:2].set(donor - passed).at[2:2 + 2 * pairs:2].set(receiver + passed)
    return lengths[jax.random.permutation(jax.random.fold_in(rng, 2), amount)]


def scatter_about(stream_key, shape, width, reach, cuts=(), kind=jnp.bfloat16):
    values = jax.random.normal(stream_key, shape, jnp.float32) * width
    if len(cuts) > 0:
        values = steps_of(stream_key, shape, cuts, -0.22, 0.18) * values
    return jnp.clip(values, min=-reach, max=reach).astype(kind)


def setup_inputs(seed: int = 0) -> dict:
    seeds = jax.random.split(jax.random.key(seed), 10)
    stream_in = scatter_about(seeds[0], (TOKENS, D), 1.0, 6.0, ((0, 32), (1, 16)))
    before_gain = jnp.clip(1.0 + 0.15 * jax.random.normal(seeds[1], (D,), jnp.float32), 0.25, 1.75).astype(jnp.bfloat16)
    after_gain = jnp.clip(1.0 + 0.15 * jax.random.normal(seeds[2], (D,), jnp.float32), 0.25, 1.75).astype(jnp.bfloat16)
    feed_gain = jnp.clip(1.0 + 0.15 * jax.random.normal(seeds[3], (D,), jnp.float32), 0.25, 1.75).astype(jnp.bfloat16)
    query_weight = draw_query_weight(jax.random.fold_in(seeds[9], 71), 0)
    key_weight = draw_key_weight(jax.random.fold_in(seeds[9], 71), 0)
    value_weight = scatter_about(seeds[6], (D, KVH * HEAD), D ** -0.5, 0.09375, ((0, 32), (1, 16)))
    output_weight = scatter_about(seeds[7], (QH * HEAD, D), (QH * HEAD) ** -0.5, 0.09375, ((0, 16), (1, 32)))
    documents = jnp.searchsorted(jnp.cumsum(uneven_parts(seeds[8], DOCS, TOKENS, LENGTH // 2, 0)), jnp.arange(TOKENS), side="right").astype(jnp.int32)
    return {"stream_in": stream_in, "before_gain": before_gain, "after_gain": after_gain, "feed_gain": feed_gain, "query_weight": query_weight, "key_weight": key_weight, "value_weight": value_weight, "output_weight": output_weight, "documents": documents}


epsilon = 1e-06
neg_big = -1e+30

def rotate(values, positions):
    half_width = values.shape[-1] // 2
    frequency = 10000.0 ** (-jnp.arange(half_width, dtype=jnp.float32) / half_width)
    angles = positions.astype(jnp.float32)[:, None] * frequency[None, :]
    cosine_table = jnp.cos(angles)[:, None, :]
    sine_table = jnp.sin(angles)[:, None, :]
    leading = values[..., :half_width]
    trailing = values[..., half_width:]
    return jnp.concatenate([leading * cosine_table - trailing * sine_table, trailing * cosine_table + leading * sine_table], axis=-1)

def norm_rows(values, gain):
    squares = lax.optimization_barrier(jnp.sum(values * values, axis=-1, keepdims=True))
    return values * lax.rsqrt(squares / D + epsilon) * gain.astype(jnp.float32)[None, :]

def reference(stream_in, before_gain, after_gain, feed_gain, query_weight, key_weight, value_weight, output_weight, documents):
    wide = stream_in.astype(jnp.float32)
    normed = norm_rows(wide, before_gain).astype(jnp.bfloat16)
    positions = (jnp.arange(TOKENS) % LENGTH).astype(jnp.int32)
    query_sum = jnp.dot(normed, query_weight, preferred_element_type=jnp.float32)
    key_sum = jnp.dot(normed, key_weight, preferred_element_type=jnp.float32)
    value_sum = jnp.dot(normed, value_weight, preferred_element_type=jnp.float32)
    queries = (rotate(query_sum.reshape(TOKENS, QH, HEAD), positions) * (D / QH) ** (-0.5)).astype(jnp.bfloat16)
    keys = rotate(key_sum.reshape(TOKENS, KVH, HEAD), positions).astype(jnp.bfloat16)
    values = value_sum.reshape(TOKENS, KVH, HEAD).astype(jnp.bfloat16)
    ratio = QH // KVH
    count_seq = TOKENS // LENGTH
    query_seq = queries.reshape(count_seq, LENGTH, KVH, ratio, HEAD)
    key_seq = keys.reshape(count_seq, LENGTH, KVH, HEAD)
    value_seq = values.reshape(count_seq, LENGTH, KVH, HEAD)
    doc_seq = documents.reshape(count_seq, LENGTH)

    def one_sequence(items):
        query_part, key_part, value_part, doc_part = items
        scores = jnp.einsum('tkrh,skh->tkrs', query_part.astype(jnp.float32), key_part.astype(jnp.float32))
        index = jnp.arange(LENGTH)
        allowed = (index[None, :] <= index[:, None]) & (doc_part[None, :] == doc_part[:, None])
        mask = allowed[:, None, None, :]
        best = lax.optimization_barrier(jnp.max(jnp.where(mask, scores, neg_big), axis=-1, keepdims=True))
        weights = jnp.where(mask, jnp.exp(scores - best), 0.0)
        total = lax.optimization_barrier(jnp.sum(weights, axis=-1))
        weights_low = lax.optimization_barrier(weights.astype(jnp.bfloat16)).astype(jnp.float32)
        summed = jnp.einsum('tkrs,skh->tkrh', weights_low, value_part.astype(jnp.float32))
        return (summed / total[..., None]).astype(jnp.bfloat16)
    attended = lax.map(one_sequence, (query_seq, key_seq, value_seq, doc_seq)).reshape(TOKENS, QH * HEAD)
    groups = N_HX * N_HY
    span = QH * HEAD // groups
    mixed = jnp.zeros((TOKENS, D), jnp.float32)
    for group in range(groups):
        term = jnp.dot(attended[:, group * span:(group + 1) * span], output_weight[group * span:(group + 1) * span, :], preferred_element_type=jnp.float32)
        mixed = mixed + lax.optimization_barrier(term.astype(jnp.bfloat16)).astype(jnp.float32)
    residual = (wide + norm_rows(mixed, after_gain)).astype(jnp.bfloat16)
    feed_input = norm_rows(residual.astype(jnp.float32), feed_gain).astype(jnp.bfloat16)
    return (residual, feed_input)
```

```python
import functools

import jax
import jax.numpy as jnp
from jax import lax
from jax.experimental import pallas as pl
from jax.experimental.pallas import tpu as pltpu
from jax.sharding import Mesh, PartitionSpec as P

D = 4608
QH = 32
HEAD = 128
LENGTH = 256
epsilon = 1e-06
neg_big = -1e30
BF, F32 = jnp.bfloat16, jnp.float32


def ring(n, s):
    return [(i, (i + s) % n) for i in range(n)]


def from_others(x, axis):
    n = lax.axis_size(axis)
    return [lax.ppermute(x, axis, ring(n, s)) for s in range(1, n)]


def copies(x, axis):
    n = lax.axis_size(axis)
    return lax.all_to_all(
        jnp.broadcast_to(x, (n, *x.shape)), axis, split_axis=0, concat_axis=0, tiled=True
    )


def norm_kernel(pos, x0, x1, x2, x3, gain, normed, first, xt, sems):
    hx, hy = pos[0], pos[1]
    n, feats = 4, 288
    moves = []
    for dy, src in enumerate((x0, x1, x2, x3)):
        for dx in range(n):
            h = ((hx + n - dx) % n) * n + (hy + n - dy) % n
            moves.append(
                pltpu.make_async_copy(
                    src.at[dx, pl.ds(0, feats)],
                    xt.at[pl.ds(pl.multiple_of(h * feats, 16), feats)],
                    sems.at[dy * n + dx],
                )
            )
    for m in moves:
        m.start()
    for m in moves:
        m.wait()
    acc = jnp.zeros((16, 256), F32)
    for b in range(D // 16):
        w = xt[b * 16 : (b + 1) * 16].astype(F32)
        acc = acc + w * w
    sq = jnp.sum(acc, axis=0, keepdims=True)
    first[...] = jnp.broadcast_to(sq, (8, 256))
    scale = lax.rsqrt(sq / D + epsilon)
    scale_col = jnp.transpose(jnp.broadcast_to(scale, (128, 256)), (1, 0))
    for b in range(D // 128):
        cols = slice(b * 128, (b + 1) * 128)
        turned = jnp.transpose(xt[cols].astype(F32), (1, 0))
        normed[:, cols] = (turned * scale_col * gain[:, cols]).astype(BF)


def attend_kernel(pos, normed, mine, other, cos, sin, mask, out, w, sems):
    c = pos[0]
    moves = []
    for t in range(16):
        moves.append(pltpu.make_async_copy(mine.at[t], w.at[t, c], sems.at[2 * t]))
        moves.append(pltpu.make_async_copy(other.at[t], w.at[t, 1 - c], sems.at[2 * t + 1]))
    for m in moves:
        m.start()
    half = D // 2
    for m in moves[:16]:
        m.wait()
    acc = jnp.dot(
        normed[:, :half], w[:8].reshape(half, 512), preferred_element_type=F32
    )
    for m in moves[16:]:
        m.wait()
    acc = acc + jnp.dot(
        normed[:, half:], w[8:].reshape(half, 512), preferred_element_type=F32
    )
    cv, sv = cos[...], sin[...]

    def rotate(u):
        a, b = u[:, :64], u[:, 64:]
        return jnp.concatenate([a * cv - b * sv, b * cv + a * sv], axis=1)

    keys = rotate(acc[:, 256:384]).astype(BF)
    values = acc[:, 384:512].astype(BF)
    allowed = mask[...] > 0.0
    for h in range(2):
        q = (rotate(acc[:, h * 128 : (h + 1) * 128]) * (D / QH) ** (-0.5)).astype(BF)
        scores = lax.dot_general(
            q, keys, (((1,), (1,)), ((), ())), preferred_element_type=F32
        )
        best = jnp.max(jnp.where(allowed, scores, neg_big), axis=1, keepdims=True)
        weights = jnp.where(allowed, jnp.exp(scores - best), 0.0)
        total = jnp.sum(weights, axis=1, keepdims=True)
        summed = jnp.dot(weights.astype(BF), values, preferred_element_type=F32)
        out[:, h * 128 : (h + 1) * 128] = (summed / total).astype(BF)


def output_kernel(pos, a0, a1, a2, a3, mine, other, x, gain, mixed, sums, att, w, sems, wsems):
    hx, hy, c = pos[0], pos[1], pos[2]
    n = 4
    moves = []
    for dy, src in enumerate((a0, a1, a2, a3)):
        for dx in range(n):
            h = ((hx + n - dx) % n) * n + (hy + n - dy) % n
            moves.append(
                pltpu.make_async_copy(src.at[dx], att.at[h], sems.at[dy * n + dx])
            )
    for t in range(16):
        moves.append(pltpu.make_async_copy(mine.at[t], w.at[t, c], wsems.at[2 * t]))
        moves.append(pltpu.make_async_copy(other.at[t], w.at[t, 1 - c], wsems.at[2 * t + 1]))
    for m in moves:
        m.start()
    for m in moves:
        m.wait()
    total = jnp.zeros((288, 256), F32)
    for g in range(16):
        term = lax.dot_general(
            w[g].reshape(288, 256), att[g], (((1,), (1,)), ((), ())), preferred_element_type=F32
        )
        total = total + term.astype(BF).astype(F32)
    mixed[...] = total
    branch = total * gain[...]
    wide = x[...].astype(F32)
    sums[0:1] = jnp.sum(total * total, axis=0, keepdims=True)
    sums[1:2] = jnp.sum(wide * branch, axis=0, keepdims=True)
    sums[2:3] = jnp.sum(branch * branch, axis=0, keepdims=True)
    sums[3:8] = jnp.zeros((5, 256), F32)


HBM = pl.BlockSpec(memory_space=pltpu.HBM)
VMEM = pl.BlockSpec(memory_space=pltpu.VMEM)
SMEM = pl.BlockSpec(memory_space=pltpu.SMEM)
params = functools.partial(pltpu.CompilerParams, vmem_limit_bytes=48 << 20)


def per_device(
    stream_in,
    before_gain,
    after_gain,
    feed_gain,
    query_weight,
    key_weight,
    value_weight,
    output_weight,
    documents,
):
    hid = ("hx", "hy")
    tok = ("yl", "z")
    hx, hy, c = lax.axis_index("hx"), lax.axis_index("hy"), lax.axis_index("c")
    pos_h = jnp.stack([hx, hy, c]).astype(jnp.int32)
    pos_c = jnp.stack([c]).astype(jnp.int32)
    rows = LENGTH

    w = jnp.concatenate([query_weight, key_weight, value_weight], axis=1)
    w_mine = copies(w, tok)
    w_other = lax.ppermute(w_mine, "c", ring(2, 1))

    x_t = stream_in.T
    gain_rows = jnp.pad(before_gain, (0, 16 * 256 - 288)).reshape(16, 256)
    packed = jnp.concatenate([x_t, gain_rows], axis=0)
    column = jnp.stack([packed, *from_others(packed, "hx")])
    parts = [column, *from_others(column, "hy")]
    gains = jnp.stack([p[:, 288:290].reshape(4, 512)[:, :288] for p in parts])
    gains = jnp.roll(gains[::-1, ::-1], (hy + 1, hx + 1), axis=(0, 1))
    gain_row = jnp.swapaxes(gains, 0, 1).reshape(1, D).astype(F32)
    normed, first = pl.pallas_call(
        norm_kernel,
        out_shape=(
            jax.ShapeDtypeStruct((rows, D), BF),
            jax.ShapeDtypeStruct((8, rows), F32),
        ),
        in_specs=[SMEM, HBM, HBM, HBM, HBM, VMEM],
        out_specs=(VMEM, VMEM),
        scratch_shapes=[pltpu.VMEM((D, rows), BF), pltpu.SemaphoreType.DMA((16,))],
        compiler_params=params(),
        name="norm_stream",
    )(pos_h, *parts, gain_row)

    half_width = HEAD // 2
    frequency = 10000.0 ** (-jnp.arange(half_width, dtype=F32) / half_width)
    angles = (jnp.arange(rows, dtype=jnp.int32) % LENGTH).astype(F32)[:, None] * frequency[None, :]
    index = jnp.arange(rows)
    mask = (
        (index[None, :] <= index[:, None]) & (documents[None, :] == documents[:, None])
    ).astype(F32)
    attended = pl.pallas_call(
        attend_kernel,
        out_shape=jax.ShapeDtypeStruct((rows, 256), BF),
        in_specs=[SMEM, VMEM, HBM, HBM, VMEM, VMEM, VMEM],
        out_specs=VMEM,
        scratch_shapes=[pltpu.VMEM((16, 2, 144, 512), BF), pltpu.SemaphoreType.DMA((32,))],
        compiler_params=params(),
        name="attend",
    )(pos_c, normed, w_mine, w_other, jnp.cos(angles), jnp.sin(angles), mask)

    turn = [
        ((a * 16 + b) * 2 + k, (b * 16 + a) * 2 + k)
        for a in range(16)
        for b in range(16)
        for k in range(2)
    ]
    wo = lax.ppermute(output_weight.T, ("hx", "hy", "yl", "z", "c"), turn)
    wo, _ = lax.optimization_barrier((wo, w_mine))
    wo_mine = copies(wo, tok)
    wo_other = lax.ppermute(wo_mine, "c", ring(2, 1))

    a_column = jnp.stack([attended, *from_others(attended, "hx")])
    a_parts = [a_column, *from_others(a_column, "hy")]
    after_col = after_gain.astype(F32)[:, None]
    feed_col = feed_gain.astype(F32)[:, None]
    mixed, sums = pl.pallas_call(
        output_kernel,
        out_shape=(
            jax.ShapeDtypeStruct((288, rows), F32),
            jax.ShapeDtypeStruct((8, rows), F32),
        ),
        in_specs=[SMEM, HBM, HBM, HBM, HBM, HBM, HBM, VMEM, VMEM],
        out_specs=(VMEM, VMEM),
        scratch_shapes=[
            pltpu.VMEM((16, rows, 256), BF),
            pltpu.VMEM((16, 2, 144, 256), BF),
            pltpu.SemaphoreType.DMA((16,)),
            pltpu.SemaphoreType.DMA((32,)),
        ],
        compiler_params=params(),
        name="project_out",
    )(pos_h, *a_parts, wo_mine, wo_other, x_t, after_col)

    for axis in ("hx", "hy"):
        got = from_others(sums, axis)
        sums = sums + got[0] + got[1] + got[2]
    after_sq, cross_sum, branch_sq = sums[0:1], sums[1:2], sums[2:3]
    first_sq = first[0:1]
    after_scale = lax.rsqrt(after_sq / D + epsilon)
    wide = x_t.astype(F32)
    residual = (wide + mixed * after_scale * after_col).astype(BF)
    feed_sq = first_sq + 2.0 * after_scale * cross_sum + after_scale * after_scale * branch_sq
    feed_scale = lax.rsqrt(feed_sq / D + epsilon)
    feed_input = (residual.astype(F32) * feed_scale * feed_col).astype(BF)
    return (residual.T, feed_input.T)


def solution(mesh):
    fine = Mesh(mesh.devices.reshape(4, 4, 2, 8, 2), ("hx", "hy", "yl", "z", "c"))
    hid, tok = ("hx", "hy"), ("yl", "z", "c")
    in_specs = (
        P(tok, hid),
        P(hid),
        P(hid),
        P(hid),
        P(tok, hid),
        P(tok, hid),
        P(tok, hid),
        P(hid, tok),
        P(tok),
    )
    out_specs = (P(tok, hid), P(tok, hid))
    return jax.shard_map(
        per_device, mesh=fine, in_specs=in_specs, out_specs=out_specs, check_vma=False
    )
```

```python
import functools

import jax
import jax.numpy as jnp
from jax import lax
from jax.experimental import pallas as pl
from jax.experimental.pallas import tpu as pltpu
from jax.sharding import Mesh, PartitionSpec as P

D = 4608
QH = 32
HEAD = 128
LENGTH = 256
epsilon = 1e-06
neg_big = -1e30
BF, F32 = jnp.bfloat16, jnp.float32


def ring(n, s):
    return [(i, (i + s) % n) for i in range(n)]


def pair_up(x):
    return jnp.stack([x, lax.ppermute(x, "yl", ring(2, 1))])


def weight_pieces(own):
    def send(x, s):
        return lax.ppermute(x, "z", ring(8, s % 8))

    below1, above1, below2, above2 = send(own, 1), send(own, -1), send(own, 2), send(own, -2)
    near = jnp.stack([own, below1, above1, below2, above2])
    below3, above3 = send(below2, 1), send(above2, -1)
    far = jnp.stack([below3, above3, jnp.stack([send(below2[0], 2), send(above2[1], -2)])])
    return near, far, lax.ppermute(near, "c", ring(2, 1)), lax.ppermute(far, "c", ring(2, 1))


def copies(x, axis):
    n = lax.axis_size(axis)
    return lax.all_to_all(
        jnp.broadcast_to(x, (n, *x.shape)), axis, split_axis=0, concat_axis=0, tiled=True
    )


def norm_kernel(x, normed, first):
    per = 288
    acc = jnp.zeros((16, 256), F32)
    for p in range(16):
        for b in range(per // 16):
            w = x[p, b * 16 : (b + 1) * 16].astype(F32)
            acc = acc + w * w
    sq = jnp.sum(acc, axis=0, keepdims=True)
    first[...] = jnp.broadcast_to(sq, (8, 256))
    scale = lax.rsqrt(sq / D + epsilon)
    scale_col = jnp.transpose(jnp.broadcast_to(scale, (128, 256)), (1, 0))
    rows = []
    for p in range(16):
        rows += [x[p, per : per + 1].astype(F32), x[p, per + 1 : per + 2, :32].astype(F32)]
    gain = jnp.concatenate(rows, axis=1)
    for b in range(D // 128):
        cols = slice(b * 128, (b + 1) * 128)
        p, at = divmod(b * 128, per)
        if at + 128 <= per:
            block = x[p, at : at + 128]
        else:
            block = jnp.concatenate([x[p, at:per], x[p + 1, : at + 128 - per]], axis=0)
        turned = jnp.transpose(block.astype(F32), (1, 0))
        normed[:, cols] = (turned * scale_col * gain[:, cols]).astype(BF)


def place_pieces(pos, sources, target, sems):
    yl, z, c = pos[0], pos[1], pos[2]
    moves = []
    for (near, far), core in zip(sources, (c, 1 - c)):
        for src, offsets in ((near, (0, 7, 1, 6, 2)), (far, (5, 3, 4))):
            for k, dz in enumerate(offsets):
                for r in range(2):
                    t = ((yl + r) % 2) * 8 + (z + dz) % 8
                    moves.append(
                        pltpu.make_async_copy(
                            src.at[k, r], target.at[t, core], sems.at[len(moves)]
                        )
                    )
    return moves


def attend_kernel(pos, normed, m0, m1, o0, o1, cos, sin, mask, out, w, sems):
    moves = place_pieces(pos, ((m0, m1), (o0, o1)), w, sems)
    for m in moves:
        m.start()
    for m in moves:
        m.wait()
    acc = jnp.dot(normed[...], w[...].reshape(D, 512), preferred_element_type=F32)
    cv, sv = cos[...], sin[...]

    def rotate(u):
        a, b = u[:, :64], u[:, 64:]
        return jnp.concatenate([a * cv - b * sv, b * cv + a * sv], axis=1)

    keys = rotate(acc[:, 256:384]).astype(BF)
    values = acc[:, 384:512].astype(BF)
    allowed = mask[...] > 0.0
    for h in range(2):
        q = (rotate(acc[:, h * 128 : (h + 1) * 128]) * (D / QH) ** (-0.5)).astype(BF)
        scores = lax.dot_general(
            q, keys, (((1,), (1,)), ((), ())), preferred_element_type=F32
        )
        best = jnp.max(jnp.where(allowed, scores, neg_big), axis=1, keepdims=True)
        weights = jnp.where(allowed, jnp.exp(scores - best), 0.0)
        total = jnp.sum(weights, axis=1, keepdims=True)
        summed = jnp.dot(weights.astype(BF), values, preferred_element_type=F32)
        out[:, h * 128 : (h + 1) * 128] = (summed / total).astype(BF)


def output_kernel(pos, att, m0, m1, o0, o1, x, gain, mixed, sums, w, sems):
    moves = place_pieces(pos, ((m0, m1), (o0, o1)), w, sems)
    for m in moves:
        m.start()
    for m in moves:
        m.wait()
    total = jnp.zeros((288, 256), F32)
    for g in range(16):
        term = lax.dot_general(
            w[g].reshape(288, 256), att[g], (((1,), (1,)), ((), ())), preferred_element_type=F32
        )
        total = total + term.astype(BF).astype(F32)
    mixed[...] = total
    branch = total * gain[...]
    wide = x[...].astype(F32)
    sums[0:1] = jnp.sum(total * total, axis=0, keepdims=True)
    sums[1:2] = jnp.sum(wide * branch, axis=0, keepdims=True)
    sums[2:3] = jnp.sum(branch * branch, axis=0, keepdims=True)
    sums[3:8] = jnp.zeros((5, 256), F32)


HBM = pl.BlockSpec(memory_space=pltpu.HBM)
VMEM = pl.BlockSpec(memory_space=pltpu.VMEM)
SMEM = pl.BlockSpec(memory_space=pltpu.SMEM)
params = functools.partial(pltpu.CompilerParams, vmem_limit_bytes=48 << 20)


def per_device(
    stream_in,
    before_gain,
    after_gain,
    feed_gain,
    query_weight,
    key_weight,
    value_weight,
    output_weight,
    documents,
):
    hid = ("hx", "hy")
    pos = jnp.stack([lax.axis_index(a) for a in ("yl", "z", "c")]).astype(jnp.int32)
    rows = LENGTH

    w = jnp.concatenate([query_weight, key_weight, value_weight], axis=1)
    w_pieces = weight_pieces(pair_up(w))

    x_t = stream_in.T
    gain_rows = jnp.pad(before_gain, (0, 16 * 256 - 288)).reshape(16, 256)
    packed = jnp.concatenate([x_t, gain_rows], axis=0)
    stream = copies(packed, hid)
    normed, first = pl.pallas_call(
        norm_kernel,
        out_shape=(
            jax.ShapeDtypeStruct((rows, D), BF),
            jax.ShapeDtypeStruct((8, rows), F32),
        ),
        in_specs=[VMEM],
        out_specs=(VMEM, VMEM),
        compiler_params=params(),
        name="norm_stream",
    )(stream)

    turn = [
        ((a * 16 + b) * 2 + k, (b * 16 + a) * 2 + k)
        for a in range(16)
        for b in range(16)
        for k in range(2)
    ]
    wo = pair_up(lax.ppermute(output_weight.T, ("hx", "hy", "yl", "z", "c"), turn))

    half_width = HEAD // 2
    frequency = 10000.0 ** (-jnp.arange(half_width, dtype=F32) / half_width)
    angles = (jnp.arange(rows, dtype=jnp.int32) % LENGTH).astype(F32)[:, None] * frequency[None, :]
    index = jnp.arange(rows)
    mask = (
        (index[None, :] <= index[:, None]) & (documents[None, :] == documents[:, None])
    ).astype(F32)
    attended = pl.pallas_call(
        attend_kernel,
        out_shape=jax.ShapeDtypeStruct((rows, 256), BF),
        in_specs=[SMEM, VMEM, HBM, HBM, HBM, HBM, VMEM, VMEM, VMEM],
        out_specs=VMEM,
        scratch_shapes=[pltpu.VMEM((16, 2, 144, 512), BF), pltpu.SemaphoreType.DMA((32,))],
        compiler_params=params(),
        name="attend",
    )(pos, normed, *w_pieces, jnp.cos(angles), jnp.sin(angles), mask)

    wo, attended = lax.optimization_barrier((wo, attended))
    wo_pieces = weight_pieces(wo)
    gathered = copies(attended, hid)
    after_col = after_gain.astype(F32)[:, None]
    feed_col = feed_gain.astype(F32)[:, None]
    mixed, sums = pl.pallas_call(
        output_kernel,
        out_shape=(
            jax.ShapeDtypeStruct((288, rows), F32),
            jax.ShapeDtypeStruct((8, rows), F32),
        ),
        in_specs=[SMEM, VMEM, HBM, HBM, HBM, HBM, VMEM, VMEM],
        out_specs=(VMEM, VMEM),
        scratch_shapes=[pltpu.VMEM((16, 2, 144, 256), BF), pltpu.SemaphoreType.DMA((32,))],
        compiler_params=params(),
        name="project_out",
    )(pos, gathered, *wo_pieces, x_t, after_col)

    sums = copies(sums, hid).sum(axis=0)
    after_sq, cross_sum, branch_sq = sums[0:1], sums[1:2], sums[2:3]
    first_sq = first[0:1]
    after_scale = lax.rsqrt(after_sq / D + epsilon)
    wide = x_t.astype(F32)
    residual = (wide + mixed * after_scale * after_col).astype(BF)
    feed_sq = first_sq + 2.0 * after_scale * cross_sum + after_scale * after_scale * branch_sq
    feed_scale = lax.rsqrt(feed_sq / D + epsilon)
    feed_input = (residual.astype(F32) * feed_scale * feed_col).astype(BF)
    return (residual.T, feed_input.T)


def solution(mesh):
    fine = Mesh(mesh.devices.reshape(4, 4, 2, 8, 2), ("hx", "hy", "yl", "z", "c"))
    hid, tok = ("hx", "hy"), ("yl", "z", "c")
    in_specs = (
        P(tok, hid),
        P(hid),
        P(hid),
        P(hid),
        P(tok, hid),
        P(tok, hid),
        P(tok, hid),
        P(hid, tok),
        P(tok),
    )
    out_specs = (P(tok, hid), P(tok, hid))
    return jax.shard_map(
        per_device, mesh=fine, in_specs=in_specs, out_specs=out_specs, check_vma=False
    )
```

```python
import jax
import jax.numpy as jnp
from jax import lax
from jax.experimental import pallas as pl
from jax.experimental.pallas import tpu as pltpu
from jax.sharding import Mesh, PartitionSpec as P


D = 4608
QH = 32
HEAD = 128
LENGTH = 256
epsilon = 1e-06
neg_big = -1e30
BF, F32 = jnp.bfloat16, jnp.float32


def ring(n, s):
    return [(i, (i + s) % n) for i in range(n)]


def z_pieces(own):
    def send(x, s):
        return lax.ppermute(x, "z", ring(8, s % 8))

    below1, above1, below2, above2 = send(own, 1), send(own, -1), send(own, 2), send(own, -2)
    far = [send(below2, 1), send(above2, -1)]
    far += [send(below2[0], 2), send(above2[1], -2)]
    return [own, below1, above1, below2, above2], far


def other_core(pieces):
    return [lax.ppermute(p, "c", ring(2, 1)) for p in pieces]


def copies(x, axis):
    n = lax.axis_size(axis)
    return lax.all_to_all(
        jnp.broadcast_to(x, (n, *x.shape)), axis, split_axis=0, concat_axis=0, tiled=True
    )


def norm_kernel(x, normed, first):
    per = 288
    acc = jnp.zeros((16, 256), F32)
    for p in range(16):
        for b in range(per // 16):
            w = x[p, b * 16 : (b + 1) * 16].astype(F32)
            acc = acc + w * w
    sq = jnp.sum(acc, axis=0, keepdims=True)
    first[...] = jnp.broadcast_to(sq, (8, 256))
    scale = lax.rsqrt(sq / D + epsilon)
    scale_col = jnp.transpose(jnp.broadcast_to(scale, (128, 256)), (1, 0))
    rows = []
    for p in range(16):
        rows += [x[p, per : per + 1].astype(F32), x[p, per + 1 : per + 2, :32].astype(F32)]
    gain = jnp.concatenate(rows, axis=1)
    for b in range(D // 128):
        cols = slice(b * 128, (b + 1) * 128)
        p, at = divmod(b * 128, per)
        if at + 128 <= per:
            block = x[p, at : at + 128]
        else:
            block = jnp.concatenate([x[p, at:per], x[p + 1, : at + 128 - per]], axis=0)
        turned = jnp.transpose(block.astype(F32), (1, 0))
        normed[:, cols] = (turned * scale_col * gain[:, cols]).astype(BF)


OFFSETS = (0, 7, 1, 6, 2, 5, 3, 4, 4)


def slots(pos, pieces):
    yl, z = pos[0], pos[1]
    for k, (piece, dz) in enumerate(zip(pieces, OFFSETS)):
        for r in range(2):
            t = ((yl + r) % 2) * 8 + (z + dz) % 8
            if k < 7:
                yield t, piece, r
            elif r == k - 7:
                yield t, piece, None


def attend_kernel(pos, normed, cos, sin, mask, *refs):
    mine, other, (out, w) = refs[:9], refs[9:18], refs[18:]
    for pieces, core in ((mine, pos[2]), (other, 1 - pos[2])):
        for t, piece, r in slots(pos, pieces):
            w[t, core] = piece[...] if r is None else piece[r]
    acc = jnp.dot(normed[...], w[...].reshape(D, 512), preferred_element_type=F32)
    cv, sv = cos[...], sin[...]

    def rotate(u):
        a, b = u[:, :64], u[:, 64:]
        return jnp.concatenate([a * cv - b * sv, b * cv + a * sv], axis=1)

    keys = rotate(acc[:, 256:384]).astype(BF)
    values = acc[:, 384:512].astype(BF)
    allowed = mask[...] > 0.0
    for h in range(2):
        q = (rotate(acc[:, h * 128 : (h + 1) * 128]) * (D / QH) ** (-0.5)).astype(BF)
        scores = lax.dot_general(
            q, keys, (((1,), (1,)), ((), ())), preferred_element_type=F32
        )
        best = jnp.max(jnp.where(allowed, scores, neg_big), axis=1, keepdims=True)
        weights = jnp.where(allowed, jnp.exp(scores - best), 0.0)
        total = jnp.sum(weights, axis=1, keepdims=True)
        summed = jnp.dot(weights.astype(BF), values, preferred_element_type=F32)
        out[:, h * 128 : (h + 1) * 128] = (summed / total).astype(BF)


def output_kernel(pos, x, gain, att, *refs):
    pieces, (mixed, sums, rows, att_v, w_v, q_v, sems, w_sems) = refs[:9], refs[9:]
    c = pos[2]
    steps = []
    for k, (piece, dz) in enumerate(zip(pieces, OFFSETS)):
        held = w_v.at[k] if k < 7 else q_v.at[k - 7]
        w_move = pltpu.make_async_copy(piece, held, w_sems.at[k])
        w_move.start()
        for r in (0, 1) if k < 7 else (k - 7,):
            t = ((pos[0] + r) % 2) * 8 + (pos[1] + dz) % 8
            at = len(steps)
            move = pltpu.make_async_copy(att.at[t], att_v.at[at], sems.at[at])
            move.start()
            first = k >= 7 or r == 0
            steps.append((w_move if first else None, move, held, r if k < 7 else None))
    total = jnp.zeros((288, 256), F32)
    for at, (w_move, move, held, r) in enumerate(steps):
        if w_move is not None:
            w_move.wait()
        move.wait()
        both = [held[i] if r is None else held[r, i] for i in range(2)]
        term = lax.dot_general(
            jnp.concatenate(both, axis=0),
            att_v[at],
            (((1,), (1,)), ((), ())),
            preferred_element_type=F32,
        )
        total = total + term.astype(BF).astype(F32)
    rows[c] = total[:144]
    rows[1 - c] = total[144:]
    total = rows[...].reshape(288, 256)
    mixed[...] = total
    branch = total * gain[...]
    wide = x[...].astype(F32)
    sums[0:1] = jnp.sum(total * total, axis=0, keepdims=True)
    sums[1:2] = jnp.sum(wide * branch, axis=0, keepdims=True)
    sums[2:3] = jnp.sum(branch * branch, axis=0, keepdims=True)
    sums[3:8] = jnp.zeros((5, 256), F32)


ANY = pl.BlockSpec(memory_space=pl.ANY)
VMEM = pl.BlockSpec(memory_space=pltpu.VMEM)
SMEM = pl.BlockSpec(memory_space=pltpu.SMEM)


def params(mib):
    return pltpu.CompilerParams(vmem_limit_bytes=mib << 20)


def per_device(
    stream_in,
    before_gain,
    after_gain,
    feed_gain,
    query_weight,
    key_weight,
    value_weight,
    output_weight,
    documents,
):
    hid = ("hx", "hy")
    pos = jnp.stack([lax.axis_index(a) for a in ("yl", "z", "c")]).astype(jnp.int32)
    rows = LENGTH

    w = jnp.concatenate([query_weight, key_weight, value_weight], axis=1)
    w_pair = lax.ppermute(w, "yl", ring(2, 1))
    near, far = z_pieces(jnp.stack([w, w_pair]))
    w_pieces = near + far + other_core(near) + other_core(far)

    x_t = stream_in.T
    gain_rows = jnp.pad(before_gain, (0, 16 * 256 - 288)).reshape(16, 256)
    packed = jnp.concatenate([x_t, gain_rows], axis=0)
    stream = copies(packed, hid)
    normed, first = pl.pallas_call(
        norm_kernel,
        out_shape=(
            jax.ShapeDtypeStruct((rows, D), BF),
            jax.ShapeDtypeStruct((8, rows), F32),
        ),
        in_specs=[VMEM],
        out_specs=(VMEM, VMEM),
        compiler_params=params(16),
        name="norm_stream",
    )(stream)

    def turned(flip):
        turn = [
            ((a * 16 + b) * 2 + k, (b * 16 + (a ^ flip)) * 2 + k)
            for a in range(16)
            for b in range(16)
            for k in range(2)
        ]
        return lax.ppermute(output_weight.T, ("hx", "hy", "yl", "z", "c"), turn)

    wo = jnp.stack([turned(0), turned(8)])
    wo = jnp.stack([wo, *other_core([wo])], axis=1)
    wo_near, wo_far = z_pieces(wo)

    half_width = HEAD // 2
    frequency = 10000.0 ** (-jnp.arange(half_width, dtype=F32) / half_width)
    angles = (jnp.arange(rows, dtype=jnp.int32) % LENGTH).astype(F32)[:, None] * frequency[None, :]
    index = jnp.arange(rows)
    mask = (
        (index[None, :] <= index[:, None]) & (documents[None, :] == documents[:, None])
    ).astype(F32)
    attended = pl.pallas_call(
        attend_kernel,
        out_shape=jax.ShapeDtypeStruct((rows, 256), BF),
        in_specs=[SMEM] + [VMEM] * 22,
        out_specs=VMEM,
        scratch_shapes=[pltpu.VMEM((16, 2, 144, 512), BF)],
        compiler_params=params(24),
        name="attend",
    )(pos, normed, jnp.cos(angles), jnp.sin(angles), mask, *w_pieces)

    gathered = copies(attended, hid)
    after_col = after_gain.astype(F32)[:, None]
    feed_col = feed_gain.astype(F32)[:, None]
    mixed, sums = pl.pallas_call(
        output_kernel,
        out_shape=(
            jax.ShapeDtypeStruct((288, rows), F32),
            jax.ShapeDtypeStruct((8, rows), F32),
        ),
        in_specs=[SMEM, VMEM, VMEM] + [ANY] * 10,
        out_specs=(VMEM, VMEM),
        scratch_shapes=[
            pltpu.VMEM((2, 144, rows), F32),
            pltpu.VMEM((16, rows, 256), BF),
            pltpu.VMEM((7, 2, 2, 144, 256), BF),
            pltpu.VMEM((2, 2, 144, 256), BF),
            pltpu.SemaphoreType.DMA((16,)),
            pltpu.SemaphoreType.DMA((9,)),
        ],
        compiler_params=params(56),
        name="project_out",
    )(pos, x_t, after_col, gathered, *wo_near, *wo_far)

    sums = copies(sums, hid).sum(axis=0)
    after_sq, cross_sum, branch_sq = sums[0:1], sums[1:2], sums[2:3]
    first_sq = first[0:1]
    after_scale = lax.rsqrt(after_sq / D + epsilon)
    wide = x_t.astype(F32)
    residual = (wide + mixed * after_scale * after_col).astype(BF)
    feed_sq = first_sq + 2.0 * after_scale * cross_sum + after_scale * after_scale * branch_sq
    feed_scale = lax.rsqrt(feed_sq / D + epsilon)
    feed_input = (residual.astype(F32) * feed_scale * feed_col).astype(BF)
    return (residual.T, feed_input.T)


def solution(mesh):
    fine = Mesh(mesh.devices.reshape(4, 4, 2, 8, 2), ("hx", "hy", "yl", "z", "c"))
    hid, tok = ("hx", "hy"), ("yl", "z", "c")
    in_specs = (
        P(tok, hid),
        P(hid),
        P(hid),
        P(hid),
        P(tok, hid),
        P(tok, hid),
        P(tok, hid),
        P(hid, tok),
        P(tok),
    )
    out_specs = (P(tok, hid), P(tok, hid))

    return jax.shard_map(
        per_device, mesh=fine, in_specs=in_specs, out_specs=out_specs, check_vma=False
    )
```

```python
import jax
import jax.numpy as jnp
from jax import lax
from jax.experimental import pallas as pl
from jax.experimental.pallas import tpu as pltpu
from jax.sharding import Mesh, PartitionSpec as P


D = 4608
QH = 32
HEAD = 128
LENGTH = 256
epsilon = 1e-06
neg_big = -1e30
BF, F32 = jnp.bfloat16, jnp.float32


def ring(n, s):
    return [(i, (i + s) % n) for i in range(n)]


def both_cores(x):
    return jnp.stack([x, lax.ppermute(x, "c", ring(2, 1))])


def z_pieces(own):
    def send(x, s):
        up_down = [((z, c), ((z + (s if c == 0 else -s)) % 8, c)) for z in range(8) for c in range(2)]
        return lax.ppermute(x, ("z", "c"), [(2 * a + b, 2 * d + e) for (a, b), (d, e) in up_down])

    one, two = send(own, 1), send(own, 2)
    three, four = send(two, 1), send(two[0], 2)
    near = [lax.ppermute(p, "c", ring(2, 1)) for p in (one, two)]
    far = [lax.ppermute(p, "c", ring(2, 1)) for p in (three, four)]
    return [own, one, two, three, four, *near, *far]


def exchanged(x, axis):
    return lax.all_to_all(x, axis, split_axis=0, concat_axis=0, tiled=True)


def norm_kernel(x, normed, first):
    per = 288
    acc = jnp.zeros((16, 256), F32)
    for p in range(16):
        for b in range(per // 16):
            w = x[p, b * 16 : (b + 1) * 16].astype(F32)
            acc = acc + w * w
    sq = jnp.sum(acc, axis=0, keepdims=True)
    first[...] = jnp.broadcast_to(sq, (8, 256))
    scale = lax.rsqrt(sq / D + epsilon)
    scale_col = jnp.transpose(jnp.broadcast_to(scale, (128, 256)), (1, 0))
    rows = []
    for p in range(16):
        rows += [x[p, per : per + 1].astype(F32), x[p, per + 1 : per + 2, :32].astype(F32)]
    gain = jnp.concatenate(rows, axis=1)
    for b in range(D // 128):
        cols = slice(b * 128, (b + 1) * 128)
        p, at = divmod(b * 128, per)
        if at + 128 <= per:
            block = x[p, at : at + 128]
        else:
            block = jnp.concatenate([x[p, at:per], x[p + 1, : at + 128 - per]], axis=0)
        turned = jnp.transpose(block.astype(F32), (1, 0))
        normed[:, cols] = (turned * scale_col * gain[:, cols]).astype(BF)


STEPS = ((0, 0), (1, 0), (2, 0), (3, 0), (4, 0), (1, 1), (2, 1), (3, 1), (4, 1))


def blocks(pos):
    yl, z, c = pos[0], pos[1], pos[2]
    for k, (far, swapped) in enumerate(STEPS):
        holder = (c + swapped) % 2
        dz = jnp.where(holder == 0, 8 - far, far)
        for i in (0, 1) if far < 4 else (0,):
            for r in range(2):
                t = ((yl + r) % 2) * 8 + (z + dz) % 8
                yield k, (i if far < 4 else None), r, t, (holder + i) % 2


def attend_kernel(pos, normed, cos, sin, mask, *refs):
    pieces, (out, w, o, sems) = refs[:9], refs[9:]
    for k, i, r, t, core in blocks(pos):
        w[t, core] = pieces[k][r] if i is None else pieces[k][i, r]
    acc = jnp.dot(normed[...], w[...].reshape(D, 512), preferred_element_type=F32)
    cv, sv = cos[...], sin[...]

    def rotate(u):
        a, b = u[:, :64], u[:, 64:]
        return jnp.concatenate([a * cv - b * sv, b * cv + a * sv], axis=1)

    keys = rotate(acc[:, 256:384]).astype(BF)
    values = acc[:, 384:512].astype(BF)
    allowed = mask[...] > 0.0
    for h in range(2):
        q = (rotate(acc[:, h * 128 : (h + 1) * 128]) * (D / QH) ** (-0.5)).astype(BF)
        scores = lax.dot_general(
            q, keys, (((1,), (1,)), ((), ())), preferred_element_type=F32
        )
        best = jnp.max(jnp.where(allowed, scores, neg_big), axis=1, keepdims=True)
        weights = jnp.where(allowed, jnp.exp(scores - best), 0.0)
        total = jnp.sum(weights, axis=1, keepdims=True)
        summed = jnp.dot(weights.astype(BF), values, preferred_element_type=F32)
        o[:, h * 128 : (h + 1) * 128] = (summed / total).astype(BF)
    moves = [pltpu.make_async_copy(o, out.at[i], sems.at[i]) for i in range(16)]
    for m in moves:
        m.start()
    for m in moves:
        m.wait()


def output_kernel(pos, x, gain, att, *refs):
    pieces, (mixed, sums, rows, att_v, *held, w_sems, sems) = refs[:9], refs[9:]
    w_moves = [pltpu.make_async_copy(p, h, w_sems.at[k]) for k, (p, h) in enumerate(zip(pieces, held))]
    moves = [pltpu.make_async_copy(att.at[g], att_v.at[g], sems.at[g]) for g in range(16)]
    for m in w_moves + moves:
        m.start()
    for m in w_moves + moves:
        m.wait()
    for k, i, r, t, core in blocks(pos):
        rows[t, core] = held[k][r] if i is None else held[k][i, r]
    total = jnp.zeros((288, 256), F32)
    for g in range(16):
        term = lax.dot_general(
            rows[g].reshape(288, 256), att_v[g], (((1,), (1,)), ((), ())), preferred_element_type=F32
        )
        total = total + term.astype(BF).astype(F32)
    mixed[...] = total
    branch = total * gain[...]
    wide = x[...].astype(F32)
    parts = [jnp.sum(u, axis=0, keepdims=True) for u in (total * total, wide * branch, branch * branch)]
    stacked = jnp.concatenate(parts + [jnp.zeros((5, 256), F32)], axis=0)
    for i in range(16):
        sums[i] = stacked


ANY = pl.BlockSpec(memory_space=pl.ANY)
VMEM = pl.BlockSpec(memory_space=pltpu.VMEM)
SMEM = pl.BlockSpec(memory_space=pltpu.SMEM)


def params(mib):
    return pltpu.CompilerParams(vmem_limit_bytes=mib << 20)


def per_device(
    stream_in,
    before_gain,
    after_gain,
    feed_gain,
    query_weight,
    key_weight,
    value_weight,
    output_weight,
    documents,
):
    hid = ("hx", "hy")
    pos = jnp.stack([lax.axis_index(a) for a in ("yl", "z", "c")]).astype(jnp.int32)
    rows = LENGTH

    w = jnp.concatenate([query_weight, key_weight, value_weight], axis=1)
    w_pair = lax.ppermute(w, "yl", ring(2, 1))
    w_pieces = z_pieces(both_cores(jnp.stack([w, w_pair])))

    x_t = stream_in.T
    gain_rows = jnp.pad(before_gain, (0, 8 * 256 - 288)).reshape(8, 256)
    packed = jnp.concatenate([x_t, gain_rows], axis=0)
    stream = exchanged(jnp.broadcast_to(packed, (16, *packed.shape)), hid)
    normed, first = pl.pallas_call(
        norm_kernel,
        out_shape=(
            jax.ShapeDtypeStruct((rows, D), BF),
            jax.ShapeDtypeStruct((8, rows), F32),
        ),
        in_specs=[VMEM],
        out_specs=(VMEM, VMEM),
        compiler_params=params(16),
        name="norm_stream",
    )(stream)

    def turned(flip):
        turn = [
            ((a * 16 + b) * 2 + k, (b * 16 + (a ^ flip)) * 2 + k)
            for a in range(16)
            for b in range(16)
            for k in range(2)
        ]
        return lax.ppermute(output_weight.T, ("hx", "hy", "yl", "z", "c"), turn)

    wo = jnp.stack([turned(0), turned(8)])
    wo_pieces = z_pieces(both_cores(wo))

    half_width = HEAD // 2
    frequency = 10000.0 ** (-jnp.arange(half_width, dtype=F32) / half_width)
    angles = (jnp.arange(rows, dtype=jnp.int32) % LENGTH).astype(F32)[:, None] * frequency[None, :]
    index = jnp.arange(rows)
    mask = (
        (index[None, :] <= index[:, None]) & (documents[None, :] == documents[:, None])
    ).astype(F32)
    attended = pl.pallas_call(
        attend_kernel,
        out_shape=jax.ShapeDtypeStruct((16, rows, 256), BF),
        in_specs=[SMEM] + [VMEM] * 13,
        out_specs=ANY,
        scratch_shapes=[
            pltpu.VMEM((16, 2, 144, 512), BF),
            pltpu.VMEM((rows, 256), BF),
            pltpu.SemaphoreType.DMA((16,)),
        ],
        compiler_params=params(24),
        name="attend",
    )(pos, normed, jnp.cos(angles), jnp.sin(angles), mask, *w_pieces)

    gathered = exchanged(attended, hid)
    after_col = after_gain.astype(F32)[:, None]
    feed_col = feed_gain.astype(F32)[:, None]
    mixed, sums = pl.pallas_call(
        output_kernel,
        out_shape=(
            jax.ShapeDtypeStruct((288, rows), F32),
            jax.ShapeDtypeStruct((16, 8, rows), F32),
        ),
        in_specs=[SMEM, VMEM, VMEM] + [ANY] * 10,
        out_specs=(VMEM, VMEM),
        scratch_shapes=[
            pltpu.VMEM((16, 2, 144, 256), BF),
            pltpu.VMEM((16, rows, 256), BF),
            *[pltpu.VMEM(p.shape, BF) for p in wo_pieces],
            pltpu.SemaphoreType.DMA((9,)),
            pltpu.SemaphoreType.DMA((16,)),
        ],
        compiler_params=params(56),
        name="project_out",
    )(pos, x_t, after_col, gathered, *wo_pieces)

    sums = exchanged(sums, hid).sum(axis=0)
    after_sq, cross_sum, branch_sq = sums[0:1], sums[1:2], sums[2:3]
    first_sq = first[0:1]
    after_scale = lax.rsqrt(after_sq / D + epsilon)
    wide = x_t.astype(F32)
    residual = (wide + mixed * after_scale * after_col).astype(BF)
    feed_sq = first_sq + 2.0 * after_scale * cross_sum + after_scale * after_scale * branch_sq
    feed_scale = lax.rsqrt(feed_sq / D + epsilon)
    feed_input = (residual.astype(F32) * feed_scale * feed_col).astype(BF)
    return (residual.T, feed_input.T)


def solution(mesh):
    fine = Mesh(mesh.devices.reshape(4, 4, 2, 8, 2), ("hx", "hy", "yl", "z", "c"))
    hid, tok = ("hx", "hy"), ("yl", "z", "c")
    in_specs = (
        P(tok, hid),
        P(hid),
        P(hid),
        P(hid),
        P(tok, hid),
        P(tok, hid),
        P(tok, hid),
        P(hid, tok),
        P(tok),
    )
    out_specs = (P(tok, hid), P(tok, hid))

    return jax.shard_map(per_device, mesh=fine, in_specs=in_specs, out_specs=out_specs, check_vma=False)
```

```python
import jax
import jax.numpy as jnp
from jax import lax
from jax.experimental import pallas as pl
from jax.experimental.pallas import tpu as pltpu
from jax.sharding import Mesh, PartitionSpec as P


D = 4608
QH = 32
HEAD = 128
LENGTH = 256
epsilon = 1e-06
neg_big = -1e30
BF, F32 = jnp.bfloat16, jnp.float32


def ring(n, s):
    return [(i, (i + s) % n) for i in range(n)]


def both_cores(x):
    return jnp.stack([x, lax.ppermute(x, "c", ring(2, 1))])


def z_pieces(own):
    def send(x, s):
        up_down = [((z, c), ((z + (s if c == 0 else -s)) % 8, c)) for z in range(8) for c in range(2)]
        return lax.ppermute(x, ("z", "c"), [(2 * a + b, 2 * d + e) for (a, b), (d, e) in up_down])

    one, two = send(own, 1), send(own, 2)
    three, four = send(two, 1), send(two[0], 2)
    near = [lax.ppermute(p, "c", ring(2, 1)) for p in (one, two)]
    far = [lax.ppermute(p, "c", ring(2, 1)) for p in (three, four)]
    return [own, one, two, three, four, *near, *far]


def exchanged(x, axis):
    return lax.all_to_all(x, axis, split_axis=0, concat_axis=0, tiled=True)


def norm_kernel(stream, normed, first):
    per = 288
    x = [stream.at[p % 4, p // 4] for p in range(16)]
    acc = jnp.zeros((16, 256), F32)
    for p in range(16):
        for b in range(per // 16):
            w = x[p][b * 16 : (b + 1) * 16].astype(F32)
            acc = acc + w * w
    sq = jnp.sum(acc, axis=0, keepdims=True)
    first[...] = jnp.broadcast_to(sq, (8, 256))
    scale = lax.rsqrt(sq / D + epsilon)
    scale_col = jnp.transpose(jnp.broadcast_to(scale, (128, 256)), (1, 0))
    rows = []
    for p in range(16):
        rows += [x[p][per : per + 1].astype(F32), x[p][per + 1 : per + 2, :32].astype(F32)]
    gain = jnp.concatenate(rows, axis=1)
    for b in range(D // 128):
        cols = slice(b * 128, (b + 1) * 128)
        p, at = divmod(b * 128, per)
        if at + 128 <= per:
            block = x[p][at : at + 128]
        else:
            block = jnp.concatenate([x[p][at:per], x[p + 1][: at + 128 - per]], axis=0)
        turned = jnp.transpose(block.astype(F32), (1, 0))
        normed[:, cols] = (turned * scale_col * gain[:, cols]).astype(BF)


STEPS = ((0, 0), (1, 0), (2, 0), (3, 0), (4, 0), (1, 1), (2, 1), (3, 1), (4, 1))


def blocks(pos):
    yl, z, c = pos[0], pos[1], pos[2]
    for k, (far, swapped) in enumerate(STEPS):
        holder = (c + swapped) % 2
        dz = jnp.where(holder == 0, 8 - far, far)
        for i in (0, 1) if far < 4 else (0,):
            for r in range(2):
                t = ((yl + r) % 2) * 8 + (z + dz) % 8
                yield k, (i if far < 4 else None), r, t, (holder + i) % 2


def attend_kernel(pos, normed, cos, sin, mask, *refs):
    pieces, (out, w, o, sems) = refs[:9], refs[9:]
    for k, i, r, t, core in blocks(pos):
        w[t, core] = pieces[k][r] if i is None else pieces[k][i, r]
    acc = jnp.dot(normed[...], w[...].reshape(D, 512), preferred_element_type=F32)
    cv, sv = cos[...], sin[...]

    def rotate(u):
        a, b = u[:, :64], u[:, 64:]
        return jnp.concatenate([a * cv - b * sv, b * cv + a * sv], axis=1)

    keys = rotate(acc[:, 256:384]).astype(BF)
    values = acc[:, 384:512].astype(BF)
    allowed = mask[...] > 0.0
    for h in range(2):
        q = (rotate(acc[:, h * 128 : (h + 1) * 128]) * (D / QH) ** (-0.5)).astype(BF)
        scores = lax.dot_general(
            q, keys, (((1,), (1,)), ((), ())), preferred_element_type=F32
        )
        best = jnp.max(jnp.where(allowed, scores, neg_big), axis=1, keepdims=True)
        weights = jnp.where(allowed, jnp.exp(scores - best), 0.0)
        total = jnp.sum(weights, axis=1, keepdims=True)
        summed = jnp.dot(weights.astype(BF), values, preferred_element_type=F32)
        o[:, h * 128 : (h + 1) * 128] = (summed / total).astype(BF)
    moves = [pltpu.make_async_copy(o, out.at[i], sems.at[i]) for i in range(4)]
    for m in moves:
        m.start()
    for m in moves:
        m.wait()


def output_kernel(pos, x, gain, att, *refs):
    pieces, (mixed, sums, rows, att_v, *held, w_sems, sems) = refs[:9], refs[9:]
    w_moves = [pltpu.make_async_copy(p, h, w_sems.at[k]) for k, (p, h) in enumerate(zip(pieces, held))]
    moves = [pltpu.make_async_copy(att.at[g % 4, g // 4], att_v.at[g], sems.at[g]) for g in range(16)]
    for m in w_moves + moves:
        m.start()
    for m in w_moves + moves:
        m.wait()
    for k, i, r, t, core in blocks(pos):
        rows[t, core] = held[k][r] if i is None else held[k][i, r]
    total = jnp.zeros((288, 256), F32)
    for g in range(16):
        term = lax.dot_general(
            rows[g].reshape(288, 256), att_v[g], (((1,), (1,)), ((), ())), preferred_element_type=F32
        )
        total = total + term.astype(BF).astype(F32)
    mixed[...] = total
    branch = total * gain[...]
    wide = x[...].astype(F32)
    parts = [jnp.sum(u, axis=0, keepdims=True) for u in (total * total, wide * branch, branch * branch)]
    stacked = jnp.concatenate(parts + [jnp.zeros((5, 256), F32)], axis=0)
    for i in range(16):
        sums[i] = stacked


ANY = pl.BlockSpec(memory_space=pl.ANY)
VMEM = pl.BlockSpec(memory_space=pltpu.VMEM)
SMEM = pl.BlockSpec(memory_space=pltpu.SMEM)


def params(mib):
    return pltpu.CompilerParams(vmem_limit_bytes=mib << 20)


def per_device(
    stream_in,
    before_gain,
    after_gain,
    feed_gain,
    query_weight,
    key_weight,
    value_weight,
    output_weight,
    documents,
):
    hid = ("hx", "hy")
    pos = jnp.stack([lax.axis_index(a) for a in ("yl", "z", "c")]).astype(jnp.int32)
    rows = LENGTH

    w = jnp.concatenate([query_weight, key_weight, value_weight], axis=1)
    w_pair = lax.ppermute(w, "yl", ring(2, 1))
    w_pieces = z_pieces(both_cores(jnp.stack([w, w_pair])))

    x_t = stream_in.T
    gain_rows = jnp.pad(before_gain, (0, 8 * 256 - 288)).reshape(8, 256)
    packed = jnp.concatenate([x_t, gain_rows], axis=0)[None]
    column = exchanged(jnp.broadcast_to(packed, (4, *packed.shape[1:])), "hx")
    stream = exchanged(jnp.broadcast_to(column, (4, *column.shape)), "hy")
    normed, first = pl.pallas_call(
        norm_kernel,
        out_shape=(
            jax.ShapeDtypeStruct((rows, D), BF),
            jax.ShapeDtypeStruct((8, rows), F32),
        ),
        in_specs=[VMEM],
        out_specs=(VMEM, VMEM),
        compiler_params=params(16),
        name="norm_stream",
    )(stream.reshape(4, 4, 296, rows))

    def turned(flip):
        turn = [
            ((a * 16 + b) * 2 + k, (b * 16 + (a ^ flip)) * 2 + k)
            for a in range(16)
            for b in range(16)
            for k in range(2)
        ]
        return lax.ppermute(output_weight.T, ("hx", "hy", "yl", "z", "c"), turn)

    wo = jnp.stack([turned(0), turned(8)])
    wo_pieces = z_pieces(both_cores(wo))

    half_width = HEAD // 2
    frequency = 10000.0 ** (-jnp.arange(half_width, dtype=F32) / half_width)
    angles = (jnp.arange(rows, dtype=jnp.int32) % LENGTH).astype(F32)[:, None] * frequency[None, :]
    index = jnp.arange(rows)
    mask = (
        (index[None, :] <= index[:, None]) & (documents[None, :] == documents[:, None])
    ).astype(F32)
    attended = pl.pallas_call(
        attend_kernel,
        out_shape=jax.ShapeDtypeStruct((4, rows, 256), BF),
        in_specs=[SMEM] + [VMEM] * 13,
        out_specs=ANY,
        scratch_shapes=[
            pltpu.VMEM((16, 2, 144, 512), BF),
            pltpu.VMEM((rows, 256), BF),
            pltpu.SemaphoreType.DMA((4,)),
        ],
        compiler_params=params(24),
        name="attend",
    )(pos, normed, jnp.cos(angles), jnp.sin(angles), mask, *w_pieces)

    att_column = exchanged(attended, "hx")
    gathered = exchanged(jnp.broadcast_to(att_column, (4, *att_column.shape)), "hy")
    gathered = gathered.reshape(4, 4, rows, 256)
    after_col = after_gain.astype(F32)[:, None]
    feed_col = feed_gain.astype(F32)[:, None]
    mixed, sums = pl.pallas_call(
        output_kernel,
        out_shape=(
            jax.ShapeDtypeStruct((288, rows), F32),
            jax.ShapeDtypeStruct((16, 8, rows), F32),
        ),
        in_specs=[SMEM, VMEM, VMEM] + [ANY] * 10,
        out_specs=(VMEM, VMEM),
        scratch_shapes=[
            pltpu.VMEM((16, 2, 144, 256), BF),
            pltpu.VMEM((16, rows, 256), BF),
            *[pltpu.VMEM(p.shape, BF) for p in wo_pieces],
            pltpu.SemaphoreType.DMA((9,)),
            pltpu.SemaphoreType.DMA((16,)),
        ],
        compiler_params=params(56),
        name="project_out",
    )(pos, x_t, after_col, gathered, *wo_pieces)

    sums = exchanged(sums, hid).sum(axis=0)
    after_sq, cross_sum, branch_sq = sums[0:1], sums[1:2], sums[2:3]
    first_sq = first[0:1]
    after_scale = lax.rsqrt(after_sq / D + epsilon)
    wide = x_t.astype(F32)
    residual = (wide + mixed * after_scale * after_col).astype(BF)
    feed_sq = first_sq + 2.0 * after_scale * cross_sum + after_scale * after_scale * branch_sq
    feed_scale = lax.rsqrt(feed_sq / D + epsilon)
    feed_input = (residual.astype(F32) * feed_scale * feed_col).astype(BF)
    return (residual.T, feed_input.T)


def solution(mesh):
    fine = Mesh(mesh.devices.reshape(4, 4, 2, 8, 2), ("hx", "hy", "yl", "z", "c"))
    hid, tok = ("hx", "hy"), ("yl", "z", "c")
    in_specs = (
        P(tok, hid),
        P(hid),
        P(hid),
        P(hid),
        P(tok, hid),
        P(tok, hid),
        P(tok, hid),
        P(hid, tok),
        P(tok),
    )
    out_specs = (P(tok, hid), P(tok, hid))

    return jax.shard_map(per_device, mesh=fine, in_specs=in_specs, out_specs=out_specs, check_vma=False)
```

```python
import jax
import jax.numpy as jnp
from jax import lax
from jax.experimental import pallas as pl
from jax.experimental.pallas import tpu as pltpu
from jax.sharding import Mesh, PartitionSpec as P


D = 4608
QH = 32
HEAD = 128
LENGTH = 256
epsilon = 1e-06
neg_big = -1e30
BF, F32 = jnp.bfloat16, jnp.float32


def ring(n, s):
    return [(i, (i + s) % n) for i in range(n)]


def both_cores(x):
    return jnp.stack([x, lax.ppermute(x, "c", ring(2, 1))])


def z_pieces(own):
    def send(x, s):
        up_down = [((z, c), ((z + (s if c == 0 else -s)) % 8, c)) for z in range(8) for c in range(2)]
        return lax.ppermute(x, ("z", "c"), [(2 * a + b, 2 * d + e) for (a, b), (d, e) in up_down])

    one, two = send(own, 1), send(own, 2)
    three, four = send(two, 1), send(two[0], 2)
    near = [lax.ppermute(p, "c", ring(2, 1)) for p in (one, two)]
    far = [lax.ppermute(p, "c", ring(2, 1)) for p in (three, four)]
    return [own, one, two, three, four, *near, *far]


def exchanged(x, axis):
    return lax.all_to_all(x, axis, split_axis=0, concat_axis=0, tiled=True)


def pack_kernel(q, k, v, x, gain, w, packed, g, last, sems):
    get = pltpu.make_async_copy(gain, g, sems.at[0])
    moves = [
        pltpu.make_async_copy(q, w.at[:, pl.ds(0, 256)], sems.at[1]),
        pltpu.make_async_copy(k, w.at[:, pl.ds(256, 128)], sems.at[2]),
        pltpu.make_async_copy(v, w.at[:, pl.ds(384, 128)], sems.at[3]),
    ]
    moves += [pltpu.make_async_copy(x, packed.at[i, pl.ds(0, 288)], sems.at[4 + i]) for i in range(4)]
    get.start()
    for m in moves:
        m.start()
    get.wait()
    row = g[...].astype(F32).reshape(1, 288)
    tail = jnp.concatenate([row[:, 256:], jnp.zeros((1, 224), F32)], axis=1)
    last[...] = jnp.concatenate([row[:, :256], tail, jnp.zeros((6, 256), F32)], axis=0).astype(BF)
    ends = [pltpu.make_async_copy(last, packed.at[i, pl.ds(288, 8)], sems.at[8 + i]) for i in range(4)]
    for m in ends:
        m.start()
    for m in moves + ends:
        m.wait()


def norm_kernel(stream, normed, first):
    per = 288
    x = [stream.at[p % 4, p // 4] for p in range(16)]
    acc = jnp.zeros((16, 256), F32)
    for p in range(16):
        for b in range(per // 16):
            w = x[p][b * 16 : (b + 1) * 16].astype(F32)
            acc = acc + w * w
    sq = jnp.sum(acc, axis=0, keepdims=True)
    first[...] = jnp.broadcast_to(sq, (8, 256))
    scale = lax.rsqrt(sq / D + epsilon)
    scale_col = jnp.transpose(jnp.broadcast_to(scale, (128, 256)), (1, 0))
    rows = []
    for p in range(16):
        rows += [x[p][per : per + 1].astype(F32), x[p][per + 1 : per + 2, :32].astype(F32)]
    gain = jnp.concatenate(rows, axis=1)
    for b in range(D // 128):
        cols = slice(b * 128, (b + 1) * 128)
        p, at = divmod(b * 128, per)
        if at + 128 <= per:
            block = x[p][at : at + 128]
        else:
            block = jnp.concatenate([x[p][at:per], x[p + 1][: at + 128 - per]], axis=0)
        turned = jnp.transpose(block.astype(F32), (1, 0))
        normed[:, cols] = (turned * scale_col * gain[:, cols]).astype(BF)


STEPS = ((0, 0), (1, 0), (2, 0), (3, 0), (4, 0), (1, 1), (2, 1), (3, 1), (4, 1))


def blocks(pos):
    yl, z, c = pos[0], pos[1], pos[2]
    for k, (far, swapped) in enumerate(STEPS):
        holder = (c + swapped) % 2
        dz = jnp.where(holder == 0, 8 - far, far)
        for i in (0, 1) if far < 4 else (0,):
            for r in range(2):
                t = ((yl + r) % 2) * 8 + (z + dz) % 8
                yield k, (i if far < 4 else None), r, t, (holder + i) % 2


def attend_kernel(pos, normed, cos, sin, mask, *refs):
    pieces, (out, w, o, sems) = refs[:9], refs[9:]
    for k, i, r, t, core in blocks(pos):
        w[t, core] = pieces[k][r] if i is None else pieces[k][i, r]
    acc = jnp.dot(normed[...], w[...].reshape(D, 512), preferred_element_type=F32)
    cv, sv = cos[...], sin[...]

    def rotate(u):
        a, b = u[:, :64], u[:, 64:]
        return jnp.concatenate([a * cv - b * sv, b * cv + a * sv], axis=1)

    keys = rotate(acc[:, 256:384]).astype(BF)
    values = acc[:, 384:512].astype(BF)
    allowed = mask[...] > 0.0
    for h in range(2):
        q = (rotate(acc[:, h * 128 : (h + 1) * 128]) * (D / QH) ** (-0.5)).astype(BF)
        scores = lax.dot_general(
            q, keys, (((1,), (1,)), ((), ())), preferred_element_type=F32
        )
        best = jnp.max(jnp.where(allowed, scores, neg_big), axis=1, keepdims=True)
        weights = jnp.where(allowed, jnp.exp(scores - best), 0.0)
        total = jnp.sum(weights, axis=1, keepdims=True)
        summed = jnp.dot(weights.astype(BF), values, preferred_element_type=F32)
        o[:, h * 128 : (h + 1) * 128] = (summed / total).astype(BF)
    moves = [pltpu.make_async_copy(o, out.at[i], sems.at[i]) for i in range(4)]
    for m in moves:
        m.start()
    for m in moves:
        m.wait()


def output_kernel(pos, x, gain, att, *refs):
    pieces, (mixed, sums, rows, *held, w_sems) = refs[:9], refs[9:]
    w_moves = [pltpu.make_async_copy(p, h, w_sems.at[k]) for k, (p, h) in enumerate(zip(pieces, held))]
    for m in w_moves:
        m.start()
    for m in w_moves:
        m.wait()
    for k, i, r, t, core in blocks(pos):
        rows[t, core] = held[k][r] if i is None else held[k][i, r]
    total = jnp.zeros((288, 256), F32)
    for g in range(16):
        term = lax.dot_general(
            rows[g].reshape(288, 256),
            att[g % 4, g // 4],
            (((1,), (1,)), ((), ())),
            preferred_element_type=F32,
        )
        total = total + term.astype(BF).astype(F32)
    mixed[...] = total
    branch = total * gain[...]
    wide = x[...].astype(F32)
    parts = [jnp.sum(u, axis=0, keepdims=True) for u in (total * total, wide * branch, branch * branch)]
    stacked = jnp.concatenate(parts + [jnp.zeros((5, 256), F32)], axis=0)
    for i in range(16):
        sums[i] = stacked


ANY = pl.BlockSpec(memory_space=pl.ANY)
HBM = pl.BlockSpec(memory_space=pltpu.HBM)
VMEM = pl.BlockSpec(memory_space=pltpu.VMEM)
SMEM = pl.BlockSpec(memory_space=pltpu.SMEM)


def params(mib):
    return pltpu.CompilerParams(vmem_limit_bytes=mib << 20)


def per_device(
    stream_in,
    before_gain,
    after_gain,
    feed_gain,
    query_weight,
    key_weight,
    value_weight,
    output_weight,
    documents,
):
    hid = ("hx", "hy")
    pos = jnp.stack([lax.axis_index(a) for a in ("yl", "z", "c")]).astype(jnp.int32)
    rows = LENGTH

    x_t = stream_in.T
    w, packed = pl.pallas_call(
        pack_kernel,
        out_shape=(
            jax.ShapeDtypeStruct((144, 512), BF),
            jax.ShapeDtypeStruct((4, 296, rows), BF),
        ),
        in_specs=[HBM] * 5,
        out_specs=(HBM, HBM),
        scratch_shapes=[
            pltpu.VMEM((288,), BF),
            pltpu.VMEM((8, 256), BF),
            pltpu.SemaphoreType.DMA((12,)),
        ],
        compiler_params=params(60),
        name="pack",
    )(query_weight, key_weight, value_weight, x_t, before_gain)
    w_pair = lax.ppermute(w, "yl", ring(2, 1))
    w_pieces = z_pieces(both_cores(jnp.stack([w, w_pair])))

    column = exchanged(packed, "hx")
    stream = exchanged(jnp.broadcast_to(column, (4, *column.shape)), "hy")
    normed, first = pl.pallas_call(
        norm_kernel,
        out_shape=(
            jax.ShapeDtypeStruct((rows, D), BF),
            jax.ShapeDtypeStruct((8, rows), F32),
        ),
        in_specs=[VMEM],
        out_specs=(VMEM, VMEM),
        compiler_params=params(16),
        name="norm_stream",
    )(stream.reshape(4, 4, 296, rows))

    def turned(flip):
        turn = [
            ((a * 16 + b) * 2 + k, (b * 16 + (a ^ flip)) * 2 + k)
            for a in range(16)
            for b in range(16)
            for k in range(2)
        ]
        return lax.ppermute(output_weight.T, ("hx", "hy", "yl", "z", "c"), turn)

    wo = jnp.stack([turned(0), turned(8)])
    wo_pieces = z_pieces(both_cores(wo))

    half_width = HEAD // 2
    frequency = 10000.0 ** (-jnp.arange(half_width, dtype=F32) / half_width)
    angles = (jnp.arange(rows, dtype=jnp.int32) % LENGTH).astype(F32)[:, None] * frequency[None, :]
    index = jnp.arange(rows)
    mask = (
        (index[None, :] <= index[:, None]) & (documents[None, :] == documents[:, None])
    ).astype(F32)
    attended = pl.pallas_call(
        attend_kernel,
        out_shape=jax.ShapeDtypeStruct((4, rows, 256), BF),
        in_specs=[SMEM] + [VMEM] * 13,
        out_specs=ANY,
        scratch_shapes=[
            pltpu.VMEM((16, 2, 144, 512), BF),
            pltpu.VMEM((rows, 256), BF),
            pltpu.SemaphoreType.DMA((4,)),
        ],
        compiler_params=params(24),
        name="attend",
    )(pos, normed, jnp.cos(angles), jnp.sin(angles), mask, *w_pieces)

    att_column = exchanged(attended, "hx")
    gathered = exchanged(jnp.broadcast_to(att_column, (4, *att_column.shape)), "hy")
    gathered = gathered.reshape(4, 4, rows, 256)
    after_col = after_gain.astype(F32)[:, None]
    feed_col = feed_gain.astype(F32)[:, None]
    mixed, sums = pl.pallas_call(
        output_kernel,
        out_shape=(
            jax.ShapeDtypeStruct((288, rows), F32),
            jax.ShapeDtypeStruct((16, 8, rows), F32),
        ),
        in_specs=[SMEM] + [VMEM] * 3 + [ANY] * 9,
        out_specs=(VMEM, VMEM),
        scratch_shapes=[
            pltpu.VMEM((16, 2, 144, 256), BF),
            *[pltpu.VMEM(p.shape, BF) for p in wo_pieces],
            pltpu.SemaphoreType.DMA((9,)),
        ],
        compiler_params=params(56),
        name="project_out",
    )(pos, x_t, after_col, gathered, *wo_pieces)

    sums = exchanged(sums, hid).sum(axis=0)
    after_sq, cross_sum, branch_sq = sums[0:1], sums[1:2], sums[2:3]
    first_sq = first[0:1]
    after_scale = lax.rsqrt(after_sq / D + epsilon)
    wide = x_t.astype(F32)
    residual = (wide + mixed * after_scale * after_col).astype(BF)
    feed_sq = first_sq + 2.0 * after_scale * cross_sum + after_scale * after_scale * branch_sq
    feed_scale = lax.rsqrt(feed_sq / D + epsilon)
    feed_input = (residual.astype(F32) * feed_scale * feed_col).astype(BF)
    return (residual.T, feed_input.T)


def solution(mesh):
    fine = Mesh(mesh.devices.reshape(4, 4, 2, 8, 2), ("hx", "hy", "yl", "z", "c"))
    hid, tok = ("hx", "hy"), ("yl", "z", "c")
    in_specs = (
        P(tok, hid),
        P(hid),
        P(hid),
        P(hid),
        P(tok, hid),
        P(tok, hid),
        P(tok, hid),
        P(hid, tok),
        P(tok),
    )
    out_specs = (P(tok, hid), P(tok, hid))

    return jax.shard_map(per_device, mesh=fine, in_specs=in_specs, out_specs=out_specs, check_vma=False)
```

```python
import jax
import jax.numpy as jnp
from jax import lax
from jax.experimental import pallas as pl
from jax.experimental.pallas import tpu as pltpu
from jax.sharding import Mesh, PartitionSpec as P


D = 4608
QH = 32
HEAD = 128
LENGTH = 256
epsilon = 1e-06
neg_big = -1e30
BF, F32 = jnp.bfloat16, jnp.float32


def ring(n, s):
    return [(i, (i + s) % n) for i in range(n)]


def both_cores(x):
    return jnp.stack([x, lax.ppermute(x, "c", ring(2, 1))])


def z_pieces(own):
    def send(x, s):
        up_down = [((z, c), ((z + (s if c == 0 else -s)) % 8, c)) for z in range(8) for c in range(2)]
        return lax.ppermute(x, ("z", "c"), [(2 * a + b, 2 * d + e) for (a, b), (d, e) in up_down])

    one, two = send(own, 1), send(own, 2)
    three, four = send(two, 1), send(two[0], 2)
    near = [lax.ppermute(p, "c", ring(2, 1)) for p in (one, two)]
    far = [lax.ppermute(p, "c", ring(2, 1)) for p in (three, four)]
    return [own, one, two, three, four, *near, *far]


def exchanged(x, axis):
    return lax.all_to_all(x, axis, split_axis=0, concat_axis=0, tiled=True)


def pack_kernel(q, k, v, x, gain, w, packed, g, sems):
    get = pltpu.make_async_copy(gain, g, sems.at[0])
    moves = [
        pltpu.make_async_copy(q, w.at[:, pl.ds(0, 256)], sems.at[1]),
        pltpu.make_async_copy(k, w.at[:, pl.ds(256, 128)], sems.at[2]),
        pltpu.make_async_copy(v, w.at[:, pl.ds(384, 128)], sems.at[3]),
        pltpu.make_async_copy(x, packed.at[0, pl.ds(0, 288)], sems.at[4]),
    ]
    get.start()
    for m in moves:
        m.start()
    get.wait()
    row = g[...].astype(F32).reshape(1, 288)
    tail = jnp.concatenate([row[:, 256:], jnp.zeros((1, 224), F32)], axis=1)
    last = jnp.concatenate([row[:, :256], tail, jnp.zeros((6, 256), F32)], axis=0).astype(BF)
    for i in range(4):
        packed[i, 288:] = last
    for m in moves:
        m.wait()
    for i in range(1, 4):
        packed[i, :288] = packed[0, :288]


def norm_kernel(stream, normed, first):
    per = 288
    x = [stream.at[p % 4, p // 4] for p in range(16)]
    acc = jnp.zeros((16, 256), F32)
    for p in range(16):
        for b in range(per // 16):
            w = x[p][b * 16 : (b + 1) * 16].astype(F32)
            acc = acc + w * w
    sq = jnp.sum(acc, axis=0, keepdims=True)
    first[...] = jnp.broadcast_to(sq, (8, 256))
    scale = lax.rsqrt(sq / D + epsilon)
    scale_col = jnp.transpose(jnp.broadcast_to(scale, (128, 256)), (1, 0))
    rows = []
    for p in range(16):
        rows += [x[p][per : per + 1].astype(F32), x[p][per + 1 : per + 2, :32].astype(F32)]
    gain = jnp.concatenate(rows, axis=1)
    for b in range(D // 128):
        cols = slice(b * 128, (b + 1) * 128)
        p, at = divmod(b * 128, per)
        if at + 128 <= per:
            block = x[p][at : at + 128]
        else:
            block = jnp.concatenate([x[p][at:per], x[p + 1][: at + 128 - per]], axis=0)
        turned = jnp.transpose(block.astype(F32), (1, 0))
        normed[:, cols] = (turned * scale_col * gain[:, cols]).astype(BF)


STEPS = ((0, 0), (1, 0), (2, 0), (3, 0), (4, 0), (1, 1), (2, 1), (3, 1), (4, 1))


def blocks(pos):
    yl, z, c = pos[0], pos[1], pos[2]
    for k, (far, swapped) in enumerate(STEPS):
        holder = (c + swapped) % 2
        dz = jnp.where(holder == 0, 8 - far, far)
        for i in (0, 1) if far < 4 else (0,):
            for r in range(2):
                t = ((yl + r) % 2) * 8 + (z + dz) % 8
                yield k, (i if far < 4 else None), r, t, (holder + i) % 2


def attend_kernel(pos, normed, cos, sin, mask, *refs):
    pieces, (out, w, o, sems) = refs[:9], refs[9:]
    for k, i, r, t, core in blocks(pos):
        w[t, core] = pieces[k][r] if i is None else pieces[k][i, r]
    acc = jnp.dot(normed[...], w[...].reshape(D, 512), preferred_element_type=F32)
    cv, sv = cos[...], sin[...]

    def rotate(u):
        a, b = u[:, :64], u[:, 64:]
        return jnp.concatenate([a * cv - b * sv, b * cv + a * sv], axis=1)

    keys = rotate(acc[:, 256:384]).astype(BF)
    values = acc[:, 384:512].astype(BF)
    allowed = mask[...] > 0.0
    for h in range(2):
        q = (rotate(acc[:, h * 128 : (h + 1) * 128]) * (D / QH) ** (-0.5)).astype(BF)
        scores = lax.dot_general(
            q, keys, (((1,), (1,)), ((), ())), preferred_element_type=F32
        )
        best = jnp.max(jnp.where(allowed, scores, neg_big), axis=1, keepdims=True)
        weights = jnp.where(allowed, jnp.exp(scores - best), 0.0)
        total = jnp.sum(weights, axis=1, keepdims=True)
        summed = jnp.dot(weights.astype(BF), values, preferred_element_type=F32)
        o[:, h * 128 : (h + 1) * 128] = (summed / total).astype(BF)
    moves = [pltpu.make_async_copy(o, out.at[i], sems.at[i]) for i in range(4)]
    for m in moves:
        m.start()
    for m in moves:
        m.wait()


def output_kernel(pos, x, gain, att, *refs):
    pieces, (mixed, sums, rows, *held, w_sems) = refs[:9], refs[9:]
    w_moves = [pltpu.make_async_copy(p, h, w_sems.at[k]) for k, (p, h) in enumerate(zip(pieces, held))]
    for m in w_moves:
        m.start()
    for m in w_moves:
        m.wait()
    for k, i, r, t, core in blocks(pos):
        rows[t, core] = held[k][r] if i is None else held[k][i, r]
    total = jnp.zeros((288, 256), F32)
    for g in range(16):
        term = lax.dot_general(
            rows[g].reshape(288, 256),
            att[g % 4, g // 4],
            (((1,), (1,)), ((), ())),
            preferred_element_type=F32,
        )
        total = total + term.astype(BF).astype(F32)
    mixed[...] = total
    branch = total * gain[...]
    wide = x[...].astype(F32)
    parts = [jnp.sum(u, axis=0, keepdims=True) for u in (total * total, wide * branch, branch * branch)]
    stacked = jnp.concatenate(parts + [jnp.zeros((5, 256), F32)], axis=0)
    for i in range(16):
        sums[i] = stacked


ANY = pl.BlockSpec(memory_space=pl.ANY)
HBM = pl.BlockSpec(memory_space=pltpu.HBM)
VMEM = pl.BlockSpec(memory_space=pltpu.VMEM)
SMEM = pl.BlockSpec(memory_space=pltpu.SMEM)


def params(mib):
    return pltpu.CompilerParams(vmem_limit_bytes=mib << 20)


def per_device(
    stream_in,
    before_gain,
    after_gain,
    feed_gain,
    query_weight,
    key_weight,
    value_weight,
    output_weight,
    documents,
):
    hid = ("hx", "hy")
    pos = jnp.stack([lax.axis_index(a) for a in ("yl", "z", "c")]).astype(jnp.int32)
    rows = LENGTH

    x_t = stream_in.T
    w, packed = pl.pallas_call(
        pack_kernel,
        out_shape=(
            jax.ShapeDtypeStruct((144, 512), BF),
            jax.ShapeDtypeStruct((4, 296, rows), BF),
        ),
        in_specs=[HBM] * 5,
        out_specs=(VMEM, VMEM),
        scratch_shapes=[pltpu.VMEM((288,), BF), pltpu.SemaphoreType.DMA((5,))],
        compiler_params=params(60),
        name="pack",
    )(query_weight, key_weight, value_weight, x_t, before_gain)
    w_pair = lax.ppermute(w, "yl", ring(2, 1))
    w_pieces = z_pieces(both_cores(jnp.stack([w, w_pair])))

    column = exchanged(packed, "hx")
    stream = exchanged(jnp.broadcast_to(column, (4, *column.shape)), "hy")
    normed, first = pl.pallas_call(
        norm_kernel,
        out_shape=(
            jax.ShapeDtypeStruct((rows, D), BF),
            jax.ShapeDtypeStruct((8, rows), F32),
        ),
        in_specs=[VMEM],
        out_specs=(VMEM, VMEM),
        compiler_params=params(16),
        name="norm_stream",
    )(stream.reshape(4, 4, 296, rows))

    def turned(flip):
        turn = [
            ((a * 16 + b) * 2 + k, (b * 16 + (a ^ flip)) * 2 + k)
            for a in range(16)
            for b in range(16)
            for k in range(2)
        ]
        return lax.ppermute(output_weight.T, ("hx", "hy", "yl", "z", "c"), turn)

    wo = jnp.stack([turned(0), turned(8)])
    wo_pieces = z_pieces(both_cores(wo))

    half_width = HEAD // 2
    frequency = 10000.0 ** (-jnp.arange(half_width, dtype=F32) / half_width)
    angles = (jnp.arange(rows, dtype=jnp.int32) % LENGTH).astype(F32)[:, None] * frequency[None, :]
    index = jnp.arange(rows)
    mask = (
        (index[None, :] <= index[:, None]) & (documents[None, :] == documents[:, None])
    ).astype(F32)
    attended = pl.pallas_call(
        attend_kernel,
        out_shape=jax.ShapeDtypeStruct((4, rows, 256), BF),
        in_specs=[SMEM] + [VMEM] * 13,
        out_specs=ANY,
        scratch_shapes=[
            pltpu.VMEM((16, 2, 144, 512), BF),
            pltpu.VMEM((rows, 256), BF),
            pltpu.SemaphoreType.DMA((4,)),
        ],
        compiler_params=params(24),
        name="attend",
    )(pos, normed, jnp.cos(angles), jnp.sin(angles), mask, *w_pieces)

    att_column = exchanged(attended, "hx")
    gathered = exchanged(jnp.broadcast_to(att_column, (4, *att_column.shape)), "hy")
    gathered = gathered.reshape(4, 4, rows, 256)
    after_col = after_gain.astype(F32)[:, None]
    feed_col = feed_gain.astype(F32)[:, None]
    mixed, sums = pl.pallas_call(
        output_kernel,
        out_shape=(
            jax.ShapeDtypeStruct((288, rows), F32),
            jax.ShapeDtypeStruct((16, 8, rows), F32),
        ),
        in_specs=[SMEM] + [VMEM] * 3 + [ANY] * 9,
        out_specs=(VMEM, VMEM),
        scratch_shapes=[
            pltpu.VMEM((16, 2, 144, 256), BF),
            *[pltpu.VMEM(p.shape, BF) for p in wo_pieces],
            pltpu.SemaphoreType.DMA((9,)),
        ],
        compiler_params=params(56),
        name="project_out",
    )(pos, x_t, after_col, gathered, *wo_pieces)

    sums = exchanged(sums, hid).sum(axis=0)
    after_sq, cross_sum, branch_sq = sums[0:1], sums[1:2], sums[2:3]
    first_sq = first[0:1]
    after_scale = lax.rsqrt(after_sq / D + epsilon)
    wide = x_t.astype(F32)
    residual = (wide + mixed * after_scale * after_col).astype(BF)
    feed_sq = first_sq + 2.0 * after_scale * cross_sum + after_scale * after_scale * branch_sq
    feed_scale = lax.rsqrt(feed_sq / D + epsilon)
    feed_input = (residual.astype(F32) * feed_scale * feed_col).astype(BF)
    return (residual.T, feed_input.T)


def solution(mesh):
    fine = Mesh(mesh.devices.reshape(4, 4, 2, 8, 2), ("hx", "hy", "yl", "z", "c"))
    hid, tok = ("hx", "hy"), ("yl", "z", "c")
    in_specs = (
        P(tok, hid),
        P(hid),
        P(hid),
        P(hid),
        P(tok, hid),
        P(tok, hid),
        P(tok, hid),
        P(hid, tok),
        P(tok),
    )
    out_specs = (P(tok, hid), P(tok, hid))

    return jax.shard_map(
        per_device, mesh=fine, in_specs=in_specs, out_specs=out_specs, check_vma=False
    )
```

```python
import jax
import jax.numpy as jnp
from jax import lax
from jax.experimental import pallas as pl
from jax.experimental.pallas import tpu as pltpu
from jax.sharding import Mesh, PartitionSpec as P


D = 4608
QH = 32
HEAD = 128
LENGTH = 256
epsilon = 1e-06
neg_big = -1e30
BF, F32 = jnp.bfloat16, jnp.float32


def ring(n, s):
    return [(i, (i + s) % n) for i in range(n)]


def both_cores(x):
    return jnp.stack([x, lax.ppermute(x, "c", ring(2, 1))])


def z_pieces(own, relay):
    def send(x, s):
        up_down = [((z, c), ((z + (s if c == 0 else -s)) % 8, c)) for z in range(8) for c in range(2)]
        return lax.ppermute(x, ("z", "c"), [(2 * a + b, 2 * d + e) for (a, b), (d, e) in up_down])

    one, two = send(own, 1), send(own, 2)
    three, four = (send(two, 1), send(two[0], 2)) if relay else (send(own, 3), send(own[0], 4))
    near = [lax.ppermute(p, "c", ring(2, 1)) for p in (one, two)]
    far = [lax.ppermute(p, "c", ring(2, 1)) for p in (three, four)]
    return [own, one, two, three, four, *near, *far]


def exchanged(x, axis):
    return lax.all_to_all(x, axis, split_axis=0, concat_axis=0, tiled=True)


def pack_kernel(q, k, v, x, gain, w, packed, g, sems):
    get = pltpu.make_async_copy(gain, g, sems.at[0])
    moves = [
        pltpu.make_async_copy(q, w.at[:, pl.ds(0, 256)], sems.at[1]),
        pltpu.make_async_copy(k, w.at[:, pl.ds(256, 128)], sems.at[2]),
        pltpu.make_async_copy(v, w.at[:, pl.ds(384, 128)], sems.at[3]),
        pltpu.make_async_copy(x, packed.at[0, pl.ds(0, 288)], sems.at[4]),
    ]
    get.start()
    for m in moves:
        m.start()
    get.wait()
    row = g[...].astype(F32).reshape(1, 288)
    tail = jnp.concatenate([row[:, 256:], jnp.zeros((1, 224), F32)], axis=1)
    last = jnp.concatenate([row[:, :256], tail, jnp.zeros((6, 256), F32)], axis=0).astype(BF)
    for i in range(4):
        packed[i, 288:] = last
    for m in moves:
        m.wait()
    for i in range(1, 4):
        packed[i, :288] = packed[0, :288]


def norm_kernel(stream, normed, first):
    per = 288
    x = [stream.at[p % 4, p // 4] for p in range(16)]
    acc = jnp.zeros((16, 256), F32)
    for p in range(16):
        for b in range(per // 16):
            w = x[p][b * 16 : (b + 1) * 16].astype(F32)
            acc = acc + w * w
    sq = jnp.sum(acc, axis=0, keepdims=True)
    first[...] = jnp.broadcast_to(sq, (8, 256))
    scale = lax.rsqrt(sq / D + epsilon)
    scale_col = jnp.transpose(jnp.broadcast_to(scale, (128, 256)), (1, 0))
    rows = []
    for p in range(16):
        rows += [x[p][per : per + 1].astype(F32), x[p][per + 1 : per + 2, :32].astype(F32)]
    gain = jnp.concatenate(rows, axis=1)
    for b in range(D // 128):
        cols = slice(b * 128, (b + 1) * 128)
        p, at = divmod(b * 128, per)
        if at + 128 <= per:
            block = x[p][at : at + 128]
        else:
            block = jnp.concatenate([x[p][at:per], x[p + 1][: at + 128 - per]], axis=0)
        turned = jnp.transpose(block.astype(F32), (1, 0))
        normed[:, cols] = (turned * scale_col * gain[:, cols]).astype(BF)


STEPS = ((0, 0), (1, 0), (2, 0), (3, 0), (4, 0), (1, 1), (2, 1), (3, 1), (4, 1))


def blocks(pos):
    yl, z, c = pos[0], pos[1], pos[2]
    for k, (far, swapped) in enumerate(STEPS):
        holder = (c + swapped) % 2
        dz = jnp.where(holder == 0, 8 - far, far)
        for i in (0, 1) if far < 4 else (0,):
            for r in range(2):
                t = ((yl + r) % 2) * 8 + (z + dz) % 8
                yield k, (i if far < 4 else None), r, t, (holder + i) % 2


def attend_kernel(pos, normed, cos, sin, mask, *refs):
    pieces, (out, w, o, sems) = refs[:9], refs[9:]
    for k, i, r, t, core in blocks(pos):
        w[t, core] = pieces[k][r] if i is None else pieces[k][i, r]
    acc = jnp.dot(normed[...], w[...].reshape(D, 512), preferred_element_type=F32)
    cv, sv = cos[...], sin[...]

    def rotate(u):
        a, b = u[:, :64], u[:, 64:]
        return jnp.concatenate([a * cv - b * sv, b * cv + a * sv], axis=1)

    keys = rotate(acc[:, 256:384]).astype(BF)
    values = acc[:, 384:512].astype(BF)
    allowed = mask[...] > 0.0
    for h in range(2):
        q = (rotate(acc[:, h * 128 : (h + 1) * 128]) * (D / QH) ** (-0.5)).astype(BF)
        scores = lax.dot_general(
            q, keys, (((1,), (1,)), ((), ())), preferred_element_type=F32
        )
        best = jnp.max(jnp.where(allowed, scores, neg_big), axis=1, keepdims=True)
        weights = jnp.where(allowed, jnp.exp(scores - best), 0.0)
        total = jnp.sum(weights, axis=1, keepdims=True)
        summed = jnp.dot(weights.astype(BF), values, preferred_element_type=F32)
        o[:, h * 128 : (h + 1) * 128] = (summed / total).astype(BF)
    moves = [pltpu.make_async_copy(o, out.at[i], sems.at[i]) for i in range(4)]
    for m in moves:
        m.start()
    for m in moves:
        m.wait()


def place_kernel(pos, *refs):
    pieces, rows = refs[:9], refs[9]
    for k, i, r, t, core in blocks(pos):
        rows[t, core] = pieces[k][r] if i is None else pieces[k][i, r]


def output_kernel(x, gain, att, rows, mixed, sums):
    total = jnp.zeros((288, 256), F32)
    for g in range(16):
        term = lax.dot_general(
            rows[g].reshape(288, 256),
            att[g % 4, g // 4],
            (((1,), (1,)), ((), ())),
            preferred_element_type=F32,
        )
        total = total + term.astype(BF).astype(F32)
    mixed[...] = total
    branch = total * gain[...]
    wide = x[...].astype(F32)
    parts = [jnp.sum(u, axis=0, keepdims=True) for u in (total * total, wide * branch, branch * branch)]
    stacked = jnp.concatenate(parts + [jnp.zeros((5, 256), F32)], axis=0)
    for i in range(16):
        sums[i] = stacked


ANY = pl.BlockSpec(memory_space=pl.ANY)
HBM = pl.BlockSpec(memory_space=pltpu.HBM)
VMEM = pl.BlockSpec(memory_space=pltpu.VMEM)
SMEM = pl.BlockSpec(memory_space=pltpu.SMEM)


def params(mib):
    return pltpu.CompilerParams(vmem_limit_bytes=mib << 20)


def per_device(
    stream_in,
    before_gain,
    after_gain,
    feed_gain,
    query_weight,
    key_weight,
    value_weight,
    output_weight,
    documents,
):
    hid = ("hx", "hy")
    pos = jnp.stack([lax.axis_index(a) for a in ("yl", "z", "c")]).astype(jnp.int32)
    rows = LENGTH

    x_t = stream_in.T
    w, packed = pl.pallas_call(
        pack_kernel,
        out_shape=(
            jax.ShapeDtypeStruct((144, 512), BF),
            jax.ShapeDtypeStruct((4, 296, rows), BF),
        ),
        in_specs=[HBM] * 5,
        out_specs=(VMEM, VMEM),
        scratch_shapes=[pltpu.VMEM((288,), BF), pltpu.SemaphoreType.DMA((5,))],
        compiler_params=params(60),
        name="pack",
    )(query_weight, key_weight, value_weight, x_t, before_gain)
    w_pair = lax.ppermute(w, "yl", ring(2, 1))
    w_pieces = z_pieces(both_cores(jnp.stack([w, w_pair])), True)

    column = exchanged(packed, "hx")
    stream = exchanged(jnp.broadcast_to(column, (4, *column.shape)), "hy")
    normed, first = pl.pallas_call(
        norm_kernel,
        out_shape=(
            jax.ShapeDtypeStruct((rows, D), BF),
            jax.ShapeDtypeStruct((8, rows), F32),
        ),
        in_specs=[VMEM],
        out_specs=(VMEM, VMEM),
        compiler_params=params(16),
        name="norm_stream",
    )(stream.reshape(4, 4, 296, rows))

    def turned(flip):
        turn = [
            ((a * 16 + b) * 2 + k, (b * 16 + (a ^ flip)) * 2 + k)
            for a in range(16)
            for b in range(16)
            for k in range(2)
        ]
        return lax.ppermute(output_weight.T, ("hx", "hy", "yl", "z", "c"), turn)

    wo_here = turned(0)
    wo = jnp.stack([wo_here, turned(8)])
    wo_pieces = z_pieces(both_cores(wo), False)

    half_width = HEAD // 2
    frequency = 10000.0 ** (-jnp.arange(half_width, dtype=F32) / half_width)
    angles = (jnp.arange(rows, dtype=jnp.int32) % LENGTH).astype(F32)[:, None] * frequency[None, :]
    index = jnp.arange(rows)
    mask = (
        (index[None, :] <= index[:, None]) & (documents[None, :] == documents[:, None])
    ).astype(F32)
    attended = pl.pallas_call(
        attend_kernel,
        out_shape=jax.ShapeDtypeStruct((4, rows, 256), BF),
        in_specs=[SMEM] + [VMEM] * 13,
        out_specs=ANY,
        scratch_shapes=[
            pltpu.VMEM((16, 2, 144, 512), BF),
            pltpu.VMEM((rows, 256), BF),
            pltpu.SemaphoreType.DMA((4,)),
        ],
        compiler_params=params(24),
        name="attend",
    )(pos, normed, jnp.cos(angles), jnp.sin(angles), mask, *w_pieces)

    att_column = exchanged(attended, "hx")
    gathered = exchanged(jnp.broadcast_to(att_column, (4, *att_column.shape)), "hy")
    gathered = gathered.reshape(4, 4, rows, 256)
    after_col = after_gain.astype(F32)[:, None]
    feed_col = feed_gain.astype(F32)[:, None]
    wo_rows = pl.pallas_call(
        place_kernel,
        out_shape=jax.ShapeDtypeStruct((16, 2, 144, 256), BF),
        in_specs=[SMEM] + [VMEM] * 9,
        out_specs=VMEM,
        compiler_params=params(12),
        name="place",
    )(pos, *wo_pieces)
    mixed, sums = pl.pallas_call(
        output_kernel,
        out_shape=(
            jax.ShapeDtypeStruct((288, rows), F32),
            jax.ShapeDtypeStruct((16, 8, rows), F32),
        ),
        in_specs=[VMEM] * 4,
        out_specs=(VMEM, VMEM),
        compiler_params=params(16),
        name="project_out",
    )(x_t, after_col, gathered, wo_rows)

    sums = exchanged(sums, hid).sum(axis=0)
    after_sq, cross_sum, branch_sq = sums[0:1], sums[1:2], sums[2:3]
    first_sq = first[0:1]
    after_scale = lax.rsqrt(after_sq / D + epsilon)
    wide = x_t.astype(F32)
    residual = (wide + mixed * after_scale * after_col).astype(BF)
    feed_sq = first_sq + 2.0 * after_scale * cross_sum + after_scale * after_scale * branch_sq
    feed_scale = lax.rsqrt(feed_sq / D + epsilon)
    feed_input = (residual.astype(F32) * feed_scale * feed_col).astype(BF)
    return (residual.T, feed_input.T)


def solution(mesh):
    fine = Mesh(mesh.devices.reshape(4, 4, 2, 8, 2), ("hx", "hy", "yl", "z", "c"))
    hid, tok = ("hx", "hy"), ("yl", "z", "c")
    in_specs = (
        P(tok, hid),
        P(hid),
        P(hid),
        P(hid),
        P(tok, hid),
        P(tok, hid),
        P(tok, hid),
        P(hid, tok),
        P(tok),
    )
    out_specs = (P(tok, hid), P(tok, hid))

    return jax.shard_map(
        per_device, mesh=fine, in_specs=in_specs, out_specs=out_specs, check_vma=False
    )
```

```python
import jax
import jax.numpy as jnp
from jax import lax
from jax.experimental import pallas as pl
from jax.experimental.pallas import tpu as pltpu
from jax.sharding import Mesh, PartitionSpec as P


D = 4608
QH = 32
HEAD = 128
LENGTH = 256
epsilon = 1e-06
neg_big = -1e30
BF, F32 = jnp.bfloat16, jnp.float32


def ring(n, s):
    return [(i, (i + s) % n) for i in range(n)]


def both_cores(x):
    return jnp.stack([x, lax.ppermute(x, "c", ring(2, 1))])


def z_pieces(own, relay):
    def send(x, s):
        up_down = [((z, c), ((z + (s if c == 0 else -s)) % 8, c)) for z in range(8) for c in range(2)]
        return lax.ppermute(x, ("z", "c"), [(2 * a + b, 2 * d + e) for (a, b), (d, e) in up_down])

    two = send(own, 2)
    one = send(own, 1)
    three, four = (send(two, 1), send(two[0], 2)) if relay else (send(own, 3), send(own[0], 4))
    near = [lax.ppermute(p, "c", ring(2, 1)) for p in (one, two)]
    far = [lax.ppermute(p, "c", ring(2, 1)) for p in (three, four)]
    return [own, one, two, three, four, *near, *far]


def exchanged(x, axis):
    return lax.all_to_all(x, axis, split_axis=0, concat_axis=0, tiled=True)


def pack_kernel(q, k, v, x, gain, w, packed, g, sems):
    get = pltpu.make_async_copy(gain, g, sems.at[0])
    moves = [
        pltpu.make_async_copy(q, w.at[:, pl.ds(0, 256)], sems.at[1]),
        pltpu.make_async_copy(k, w.at[:, pl.ds(256, 128)], sems.at[2]),
        pltpu.make_async_copy(v, w.at[:, pl.ds(384, 128)], sems.at[3]),
        pltpu.make_async_copy(x, packed.at[0, pl.ds(0, 288)], sems.at[4]),
    ]
    get.start()
    for m in moves:
        m.start()
    get.wait()
    row = g[...].astype(F32).reshape(1, 288)
    tail = jnp.concatenate([row[:, 256:], jnp.zeros((1, 224), F32)], axis=1)
    last = jnp.concatenate([row[:, :256], tail, jnp.zeros((6, 256), F32)], axis=0).astype(BF)
    for i in range(4):
        packed[i, 288:] = last
    for m in moves:
        m.wait()
    for i in range(1, 4):
        packed[i, :288] = packed[0, :288]


def norm_kernel(stream, normed, first):
    per = 288
    x = [stream.at[p % 4, p // 4] for p in range(16)]
    acc = jnp.zeros((16, 256), F32)
    for p in range(16):
        for b in range(per // 16):
            w = x[p][b * 16 : (b + 1) * 16].astype(F32)
            acc = acc + w * w
    sq = jnp.sum(acc, axis=0, keepdims=True)
    first[...] = jnp.broadcast_to(sq, (8, 256))
    scale = lax.rsqrt(sq / D + epsilon)
    scale_col = jnp.transpose(jnp.broadcast_to(scale, (128, 256)), (1, 0))
    rows = []
    for p in range(16):
        rows += [x[p][per : per + 1].astype(F32), x[p][per + 1 : per + 2, :32].astype(F32)]
    gain = jnp.concatenate(rows, axis=1)
    for b in range(D // 128):
        cols = slice(b * 128, (b + 1) * 128)
        p, at = divmod(b * 128, per)
        if at + 128 <= per:
            block = x[p][at : at + 128]
        else:
            block = jnp.concatenate([x[p][at:per], x[p + 1][: at + 128 - per]], axis=0)
        turned = jnp.transpose(block.astype(F32), (1, 0))
        normed[:, cols] = (turned * scale_col * gain[:, cols]).astype(BF)


STEPS = ((0, 0), (1, 0), (2, 0), (3, 0), (4, 0), (1, 1), (2, 1), (3, 1), (4, 1))


def blocks(pos):
    yl, z, c = pos[0], pos[1], pos[2]
    for k, (far, swapped) in enumerate(STEPS):
        holder = (c + swapped) % 2
        dz = jnp.where(holder == 0, 8 - far, far)
        for i in (0, 1) if far < 4 else (0,):
            for r in range(2):
                t = ((yl + r) % 2) * 8 + (z + dz) % 8
                yield k, (i if far < 4 else None), r, t, (holder + i) % 2


def attend_kernel(pos, normed, cos, sin, mask, *refs):
    pieces, (out, w, o, sems) = refs[:9], refs[9:]
    for k, i, r, t, core in blocks(pos):
        w[t, core] = pieces[k][r] if i is None else pieces[k][i, r]
    acc = jnp.dot(normed[...], w[...].reshape(D, 512), preferred_element_type=F32)
    cv, sv = cos[...], sin[...]

    def rotate(u):
        a, b = u[:, :64], u[:, 64:]
        return jnp.concatenate([a * cv - b * sv, b * cv + a * sv], axis=1)

    keys = rotate(acc[:, 256:384]).astype(BF)
    values = acc[:, 384:512].astype(BF)
    allowed = mask[...] > 0.0
    for h in range(2):
        q = (rotate(acc[:, h * 128 : (h + 1) * 128]) * (D / QH) ** (-0.5)).astype(BF)
        scores = lax.dot_general(
            q, keys, (((1,), (1,)), ((), ())), preferred_element_type=F32
        )
        best = jnp.max(jnp.where(allowed, scores, neg_big), axis=1, keepdims=True)
        weights = jnp.where(allowed, jnp.exp(scores - best), 0.0)
        total = jnp.sum(weights, axis=1, keepdims=True)
        summed = jnp.dot(weights.astype(BF), values, preferred_element_type=F32)
        o[:, h * 128 : (h + 1) * 128] = (summed / total).astype(BF)
    moves = [pltpu.make_async_copy(o, out.at[i], sems.at[i]) for i in range(4)]
    for m in moves:
        m.start()
    for m in moves:
        m.wait()


def place_kernel(pos, *refs):
    pieces, rows = refs[:9], refs[9]
    for k, i, r, t, core in blocks(pos):
        rows[t, core] = pieces[k][r] if i is None else pieces[k][i, r]


def output_kernel(x, gain, att, rows, mixed, sums):
    total = jnp.zeros((288, 256), F32)
    for g in range(16):
        term = lax.dot_general(
            rows[g].reshape(288, 256),
            att[g % 4, g // 4],
            (((1,), (1,)), ((), ())),
            preferred_element_type=F32,
        )
        total = total + term.astype(BF).astype(F32)
    mixed[...] = total
    branch = total * gain[...]
    wide = x[...].astype(F32)
    parts = [jnp.sum(u, axis=0, keepdims=True) for u in (total * total, wide * branch, branch * branch)]
    stacked = jnp.concatenate(parts + [jnp.zeros((5, 256), F32)], axis=0)
    for i in range(16):
        sums[i] = stacked


ANY = pl.BlockSpec(memory_space=pl.ANY)
HBM = pl.BlockSpec(memory_space=pltpu.HBM)
VMEM = pl.BlockSpec(memory_space=pltpu.VMEM)
SMEM = pl.BlockSpec(memory_space=pltpu.SMEM)


def params(mib):
    return pltpu.CompilerParams(vmem_limit_bytes=mib << 20)


def per_device(
    stream_in,
    before_gain,
    after_gain,
    feed_gain,
    query_weight,
    key_weight,
    value_weight,
    output_weight,
    documents,
):
    hid = ("hx", "hy")
    pos = jnp.stack([lax.axis_index(a) for a in ("yl", "z", "c")]).astype(jnp.int32)
    rows = LENGTH

    x_t = stream_in.T
    w, packed = pl.pallas_call(
        pack_kernel,
        out_shape=(
            jax.ShapeDtypeStruct((144, 512), BF),
            jax.ShapeDtypeStruct((4, 296, rows), BF),
        ),
        in_specs=[HBM] * 5,
        out_specs=(VMEM, VMEM),
        scratch_shapes=[pltpu.VMEM((288,), BF), pltpu.SemaphoreType.DMA((5,))],
        compiler_params=params(60),
        name="pack",
    )(query_weight, key_weight, value_weight, x_t, before_gain)
    w_pair = lax.ppermute(w, "yl", ring(2, 1))
    w_pieces = z_pieces(both_cores(jnp.stack([w, w_pair])), True)

    column = exchanged(packed, "hx")
    stream = exchanged(jnp.broadcast_to(column, (4, *column.shape)), "hy")
    normed, first = pl.pallas_call(
        norm_kernel,
        out_shape=(
            jax.ShapeDtypeStruct((rows, D), BF),
            jax.ShapeDtypeStruct((8, rows), F32),
        ),
        in_specs=[VMEM],
        out_specs=(VMEM, VMEM),
        compiler_params=params(16),
        name="norm_stream",
    )(stream.reshape(4, 4, 296, rows))

    def turned(flip):
        turn = [
            ((a * 16 + b) * 2 + k, (b * 16 + (a ^ flip)) * 2 + k)
            for a in range(16)
            for b in range(16)
            for k in range(2)
        ]
        return lax.ppermute(output_weight.T, ("hx", "hy", "yl", "z", "c"), turn)

    wo_here = turned(0)
    wo = jnp.stack([wo_here, turned(8)])
    wo_pieces = z_pieces(both_cores(wo), True)

    half_width = HEAD // 2
    frequency = 10000.0 ** (-jnp.arange(half_width, dtype=F32) / half_width)
    angles = (jnp.arange(rows, dtype=jnp.int32) % LENGTH).astype(F32)[:, None] * frequency[None, :]
    index = jnp.arange(rows)
    mask = (
        (index[None, :] <= index[:, None]) & (documents[None, :] == documents[:, None])
    ).astype(F32)
    attended = pl.pallas_call(
        attend_kernel,
        out_shape=jax.ShapeDtypeStruct((4, rows, 256), BF),
        in_specs=[SMEM] + [VMEM] * 13,
        out_specs=ANY,
        scratch_shapes=[
            pltpu.VMEM((16, 2, 144, 512), BF),
            pltpu.VMEM((rows, 256), BF),
            pltpu.SemaphoreType.DMA((4,)),
        ],
        compiler_params=params(24),
        name="attend",
    )(pos, normed, jnp.cos(angles), jnp.sin(angles), mask, *w_pieces)

    att_column = exchanged(attended, "hx")
    gathered = exchanged(jnp.broadcast_to(att_column, (4, *att_column.shape)), "hy")
    gathered = gathered.reshape(4, 4, rows, 256)
    after_col = after_gain.astype(F32)[:, None]
    feed_col = feed_gain.astype(F32)[:, None]
    wo_rows = pl.pallas_call(
        place_kernel,
        out_shape=jax.ShapeDtypeStruct((16, 2, 144, 256), BF),
        in_specs=[SMEM] + [VMEM] * 9,
        out_specs=VMEM,
        compiler_params=params(12),
        name="place",
    )(pos, *wo_pieces)
    mixed, sums = pl.pallas_call(
        output_kernel,
        out_shape=(
            jax.ShapeDtypeStruct((288, rows), F32),
            jax.ShapeDtypeStruct((16, 8, rows), F32),
        ),
        in_specs=[VMEM] * 4,
        out_specs=(VMEM, VMEM),
        compiler_params=params(16),
        name="project_out",
    )(x_t, after_col, gathered, wo_rows)

    sums = exchanged(sums, hid).sum(axis=0)
    after_sq, cross_sum, branch_sq = sums[0:1], sums[1:2], sums[2:3]
    first_sq = first[0:1]
    after_scale = lax.rsqrt(after_sq / D + epsilon)
    wide = x_t.astype(F32)
    residual = (wide + mixed * after_scale * after_col).astype(BF)
    feed_sq = first_sq + 2.0 * after_scale * cross_sum + after_scale * after_scale * branch_sq
    feed_scale = lax.rsqrt(feed_sq / D + epsilon)
    feed_input = (residual.astype(F32) * feed_scale * feed_col).astype(BF)
    return (residual.T, feed_input.T)


def solution(mesh):
    fine = Mesh(mesh.devices.reshape(4, 4, 2, 8, 2), ("hx", "hy", "yl", "z", "c"))
    hid, tok = ("hx", "hy"), ("yl", "z", "c")
    in_specs = (
        P(tok, hid),
        P(hid),
        P(hid),
        P(hid),
        P(tok, hid),
        P(tok, hid),
        P(tok, hid),
        P(hid, tok),
        P(tok),
    )
    out_specs = (P(tok, hid), P(tok, hid))

    return jax.shard_map(
        per_device, mesh=fine, in_specs=in_specs, out_specs=out_specs, check_vma=False
    )
```

```python
import jax
import jax.numpy as jnp
from jax import lax
from jax.experimental import pallas as pl
from jax.experimental.pallas import tpu as pltpu
from jax.sharding import Mesh, PartitionSpec as P


D = 4608
QH = 32
HEAD = 128
LENGTH = 256
epsilon = 1e-06
neg_big = -1e30
BF, F32 = jnp.bfloat16, jnp.float32


def ring(n, s):
    return [(i, (i + s) % n) for i in range(n)]


def both_cores(x):
    return jnp.stack([x, lax.ppermute(x, "c", ring(2, 1))])


def z_pieces(own, relay):
    def send(x, s):
        up_down = [((z, c), ((z + (s if c == 0 else -s)) % 8, c)) for z in range(8) for c in range(2)]
        return lax.ppermute(x, ("z", "c"), [(2 * a + b, 2 * d + e) for (a, b), (d, e) in up_down])

    two = send(own, 2)
    one = send(own, 1)
    three, four = (send(two, 1), send(two[0], 2)) if relay else (send(own, 3), send(own[0], 4))
    near = [lax.ppermute(p, "c", ring(2, 1)) for p in (one, two)]
    far = [lax.ppermute(p, "c", ring(2, 1)) for p in (three, four)]
    return [own, one, two, three, four, *near, *far]


def exchanged(x, axis):
    return lax.all_to_all(x, axis, split_axis=0, concat_axis=0, tiled=True)


def pack_kernel(q, k, v, x, gain, w, packed, g, sems):
    get = pltpu.make_async_copy(gain, g, sems.at[0])
    moves = [
        pltpu.make_async_copy(q, w.at[:, pl.ds(0, 256)], sems.at[1]),
        pltpu.make_async_copy(k, w.at[:, pl.ds(256, 128)], sems.at[2]),
        pltpu.make_async_copy(v, w.at[:, pl.ds(384, 128)], sems.at[3]),
        pltpu.make_async_copy(x, packed.at[0, pl.ds(0, 288)], sems.at[4]),
    ]
    get.start()
    for m in moves:
        m.start()
    get.wait()
    row = g[...].astype(F32).reshape(1, 288)
    tail = jnp.concatenate([row[:, 256:], jnp.zeros((1, 224), F32)], axis=1)
    last = jnp.concatenate([row[:, :256], tail, jnp.zeros((6, 256), F32)], axis=0).astype(BF)
    for i in range(4):
        packed[i, 288:] = last
    for m in moves:
        m.wait()
    for i in range(1, 4):
        packed[i, :288] = packed[0, :288]


def norm_kernel(stream, normed, first):
    per = 288
    x = [stream.at[p % 4, p // 4] for p in range(16)]
    acc = jnp.zeros((16, 256), F32)
    for p in range(16):
        for b in range(per // 16):
            w = x[p][b * 16 : (b + 1) * 16].astype(F32)
            acc = acc + w * w
    sq = jnp.sum(acc, axis=0, keepdims=True)
    first[...] = jnp.broadcast_to(sq, (8, 256))
    scale = lax.rsqrt(sq / D + epsilon)
    scale_col = jnp.transpose(jnp.broadcast_to(scale, (128, 256)), (1, 0))
    rows = []
    for p in range(16):
        rows += [x[p][per : per + 1].astype(F32), x[p][per + 1 : per + 2, :32].astype(F32)]
    gain = jnp.concatenate(rows, axis=1)
    for b in range(D // 128):
        cols = slice(b * 128, (b + 1) * 128)
        p, at = divmod(b * 128, per)
        if at + 128 <= per:
            block = x[p][at : at + 128]
        else:
            block = jnp.concatenate([x[p][at:per], x[p + 1][: at + 128 - per]], axis=0)
        turned = jnp.transpose(block.astype(F32), (1, 0))
        normed[:, cols] = (turned * scale_col * gain[:, cols]).astype(BF)


STEPS = ((0, 0), (1, 0), (2, 0), (3, 0), (4, 0), (1, 1), (2, 1), (3, 1), (4, 1))


def blocks(pos):
    yl, z, c = pos[0], pos[1], pos[2]
    for k, (far, swapped) in enumerate(STEPS):
        holder = (c + swapped) % 2
        dz = jnp.where(holder == 0, 8 - far, far)
        for i in (0, 1) if far < 4 else (0,):
            for r in range(2):
                t = ((yl + r) % 2) * 8 + (z + dz) % 8
                yield k, (i if far < 4 else None), r, t, (holder + i) % 2


def attend_kernel(pos, normed, cos, sin, mask, *refs):
    pieces, (out, w, o, sems) = refs[:9], refs[9:]
    for k, i, r, t, core in blocks(pos):
        w[t, core] = pieces[k][r] if i is None else pieces[k][i, r]
    acc = jnp.dot(normed[...], w[...].reshape(D, 512), preferred_element_type=F32)
    cv, sv = cos[...], sin[...]

    def rotate(u):
        a, b = u[:, :64], u[:, 64:]
        return jnp.concatenate([a * cv - b * sv, b * cv + a * sv], axis=1)

    keys = rotate(acc[:, 256:384]).astype(BF)
    values = acc[:, 384:512].astype(BF)
    allowed = mask[...] > 0.0
    for h in range(2):
        q = (rotate(acc[:, h * 128 : (h + 1) * 128]) * (D / QH) ** (-0.5)).astype(BF)
        scores = lax.dot_general(
            q, keys, (((1,), (1,)), ((), ())), preferred_element_type=F32
        )
        best = jnp.max(jnp.where(allowed, scores, neg_big), axis=1, keepdims=True)
        weights = jnp.where(allowed, jnp.exp(scores - best), 0.0)
        total = jnp.sum(weights, axis=1, keepdims=True)
        summed = jnp.dot(weights.astype(BF), values, preferred_element_type=F32)
        o[:, h * 128 : (h + 1) * 128] = (summed / total).astype(BF)
    moves = [pltpu.make_async_copy(o, out.at[i], sems.at[i]) for i in range(4)]
    for m in moves:
        m.start()
    for m in moves:
        m.wait()


def place_kernel(pos, *refs):
    pieces, rows = refs[:9], refs[9]
    for k, i, r, t, core in blocks(pos):
        rows[t, core] = pieces[k][r] if i is None else pieces[k][i, r]


def output_kernel(x, gain, att, rows, mixed, sums):
    total = jnp.zeros((288, 256), F32)
    for g in range(16):
        term = lax.dot_general(
            rows[g].reshape(288, 256),
            att[g % 4, g // 4],
            (((1,), (1,)), ((), ())),
            preferred_element_type=F32,
        )
        total = total + term.astype(BF).astype(F32)
    mixed[...] = total
    branch = total * gain[...]
    wide = x[...].astype(F32)
    parts = [jnp.sum(u, axis=0, keepdims=True) for u in (total * total, wide * branch, branch * branch)]
    halves = [p[:, k : k + 128] for p in parts for k in (0, 128)]
    stacked = jnp.concatenate(halves + [jnp.zeros((2, 128), F32)], axis=0)
    for i in range(16):
        sums[i] = stacked


def finish_kernel(sums, mixed, x, first, after, feed, residual, out):
    part = sums[0]
    for i in range(1, 16):
        part = part + sums[i]
    after_sq, cross_sum, branch_sq = [
        jnp.concatenate([part[2 * k : 2 * k + 1], part[2 * k + 1 : 2 * k + 2]], axis=1) for k in range(3)
    ]
    scale = lax.rsqrt(after_sq / D + epsilon)
    low = (x[...].astype(F32) + mixed[...] * scale * after[...]).astype(BF)
    residual[...] = low
    feed_sq = first[0:1] + 2.0 * scale * cross_sum + scale * scale * branch_sq
    feed_scale = lax.rsqrt(feed_sq / D + epsilon)
    out[...] = (low.astype(F32) * feed_scale * feed[...]).astype(BF)


ANY = pl.BlockSpec(memory_space=pl.ANY)
HBM = pl.BlockSpec(memory_space=pltpu.HBM)
VMEM = pl.BlockSpec(memory_space=pltpu.VMEM)
SMEM = pl.BlockSpec(memory_space=pltpu.SMEM)


def params(mib):
    return pltpu.CompilerParams(vmem_limit_bytes=mib << 20)


def per_device(
    stream_in,
    before_gain,
    after_gain,
    feed_gain,
    query_weight,
    key_weight,
    value_weight,
    output_weight,
    documents,
):
    hid = ("hx", "hy")
    pos = jnp.stack([lax.axis_index(a) for a in ("yl", "z", "c")]).astype(jnp.int32)
    rows = LENGTH

    x_t = stream_in.T
    w, packed = pl.pallas_call(
        pack_kernel,
        out_shape=(
            jax.ShapeDtypeStruct((144, 512), BF),
            jax.ShapeDtypeStruct((4, 296, rows), BF),
        ),
        in_specs=[HBM] * 5,
        out_specs=(VMEM, VMEM),
        scratch_shapes=[pltpu.VMEM((288,), BF), pltpu.SemaphoreType.DMA((5,))],
        compiler_params=params(60),
        name="pack",
    )(query_weight, key_weight, value_weight, x_t, before_gain)
    w_pair = lax.ppermute(w, "yl", ring(2, 1))
    w_pieces = z_pieces(both_cores(jnp.stack([w, w_pair])), True)

    column = exchanged(packed, "hx")
    stream = exchanged(jnp.broadcast_to(column, (4, *column.shape)), "hy")
    normed, first = pl.pallas_call(
        norm_kernel,
        out_shape=(
            jax.ShapeDtypeStruct((rows, D), BF),
            jax.ShapeDtypeStruct((8, rows), F32),
        ),
        in_specs=[VMEM],
        out_specs=(VMEM, VMEM),
        compiler_params=params(16),
        name="norm_stream",
    )(stream.reshape(4, 4, 296, rows))

    def turned(flip):
        turn = [
            ((a * 16 + b) * 2 + k, (b * 16 + (a ^ flip)) * 2 + k)
            for a in range(16)
            for b in range(16)
            for k in range(2)
        ]
        return lax.ppermute(output_weight.T, ("hx", "hy", "yl", "z", "c"), turn)

    wo_here = turned(0)
    wo = jnp.stack([wo_here, turned(8)])
    wo_pieces = z_pieces(both_cores(wo), True)

    half_width = HEAD // 2
    frequency = 10000.0 ** (-jnp.arange(half_width, dtype=F32) / half_width)
    angles = (jnp.arange(rows, dtype=jnp.int32) % LENGTH).astype(F32)[:, None] * frequency[None, :]
    index = jnp.arange(rows)
    mask = (
        (index[None, :] <= index[:, None]) & (documents[None, :] == documents[:, None])
    ).astype(F32)
    attended = pl.pallas_call(
        attend_kernel,
        out_shape=jax.ShapeDtypeStruct((4, rows, 256), BF),
        in_specs=[SMEM] + [VMEM] * 13,
        out_specs=ANY,
        scratch_shapes=[
            pltpu.VMEM((16, 2, 144, 512), BF),
            pltpu.VMEM((rows, 256), BF),
            pltpu.SemaphoreType.DMA((4,)),
        ],
        compiler_params=params(24),
        name="attend",
    )(pos, normed, jnp.cos(angles), jnp.sin(angles), mask, *w_pieces)

    att_column = exchanged(attended, "hx")
    gathered = exchanged(jnp.broadcast_to(att_column, (4, *att_column.shape)), "hy")
    gathered = gathered.reshape(4, 4, rows, 256)
    after_col = after_gain.astype(F32)[:, None]
    feed_col = feed_gain.astype(F32)[:, None]
    wo_rows = pl.pallas_call(
        place_kernel,
        out_shape=jax.ShapeDtypeStruct((16, 2, 144, 256), BF),
        in_specs=[SMEM] + [VMEM] * 9,
        out_specs=VMEM,
        compiler_params=params(12),
        name="place",
    )(pos, *wo_pieces)
    mixed, sums = pl.pallas_call(
        output_kernel,
        out_shape=(
            jax.ShapeDtypeStruct((288, rows), F32),
            jax.ShapeDtypeStruct((16, 8, 128), F32),
        ),
        in_specs=[VMEM] * 4,
        out_specs=(VMEM, VMEM),
        compiler_params=params(16),
        name="project_out",
    )(x_t, after_col, gathered, wo_rows)

    sums = exchanged(sums, hid)
    residual, feed_input = pl.pallas_call(
        finish_kernel,
        out_shape=(jax.ShapeDtypeStruct((288, rows), BF), jax.ShapeDtypeStruct((288, rows), BF)),
        in_specs=[VMEM] * 6,
        out_specs=(VMEM, VMEM),
        compiler_params=params(8),
        name="finish",
    )(sums, mixed, x_t, first, after_col, feed_col)
    return (residual.T, feed_input.T)


def solution(mesh):
    fine = Mesh(mesh.devices.reshape(4, 4, 2, 8, 2), ("hx", "hy", "yl", "z", "c"))
    hid, tok = ("hx", "hy"), ("yl", "z", "c")
    in_specs = (
        P(tok, hid),
        P(hid),
        P(hid),
        P(hid),
        P(tok, hid),
        P(tok, hid),
        P(tok, hid),
        P(hid, tok),
        P(tok),
    )
    out_specs = (P(tok, hid), P(tok, hid))

    return jax.shard_map(
        per_device, mesh=fine, in_specs=in_specs, out_specs=out_specs, check_vma=False
    )
```
